32 devices in a mesh: freq: 8 (over z, x), kgrp: 4 (over y, core).
Axes of the slice: x: 2, y: 2, z: 4, core: 2. Of those that a mesh axis runs over, the one named last changes fastest.
Arguments:
- hamiltonian: float32 [256, 64, 128], P(('freq', 'kgrp')), may hold values from -1 to 1, as said below
- self_energy: float32 [16, 64, 128], P('freq'), may hold values from -0.8 to 0.3, as said below
- guess_factor: float32 [16, 64, 128], P('freq'), may hold values from -0.05 to 1.25
- weights: int32 [256], replicated, may hold values from 1 to 48
- counts: int32 [16], replicated, may hold values from 1 to 3, as said below
Outputs:
- local_green: float32 [4096, 32], P(('freq', 'kgrp'))
The draws below stay inside these ranges and needn't reach their ends.
Inputs may be any that keep to these rules, and one draw needn't show every extreme that they name: `hamiltonian`: each k-point's matrix is Hermitian: the left half symmetric, the right half antisymmetric. `self_energy`: the diagonal of the right half lies between -0.8 and -0.4. `counts`: the number of Newton-Schulz steps taken at each frequency.
All inputs are finite; a program needn't handle non-finite values.
Results may differ from the reference program's by a relative error of at most 0.0001.
Values sent between devices are 32-bit elements.
No kernel may reach another device: no remote copies, remote signals or barrier semaphores. Data moves between devices by JAX's collectives and lax.ppermute only.
A program may use at most 64 MiB of HBM per device.

```python
import math
import jax
import jax.numpy as jnp
from jax import lax

NORB = 64
MAXIT = 3
FREQ = 16
KPTS = 256


def noise_draw(key, shape, spread):
    return jax.random.truncated_normal(key, -4.0, 4.0, shape, jnp.float32) * spread


def draw_hamiltonian(key, part):
    first_key, second_key, third_key = jax.random.split(key, 3)
    identity = jnp.eye(NORB, dtype=jnp.float32)
    left_noise = noise_draw(first_key, (KPTS, NORB, NORB), 0.018)
    right_noise = noise_draw(second_key, (KPTS, NORB, NORB), 0.018)
    symmetric = (left_noise + jnp.swapaxes(left_noise, 1, 2)) * 0.70710678 * (1.0 - identity)
    skewed = (right_noise - jnp.swapaxes(right_noise, 1, 2)) * 0.70710678
    levels = jax.random.uniform(third_key, (KPTS, NORB), jnp.float32, -1.0, 1.0)
    real_part = symmetric + levels[:, :, None] * identity
    return jnp.concatenate([real_part, skewed], -1).astype(jnp.float32)


def draw_self_energy(key, part):
    first_key, second_key, third_key, fourth_key = jax.random.split(key, 4)
    identity = jnp.eye(NORB, dtype=jnp.float32)
    real_off = noise_draw(first_key, (FREQ, NORB, NORB), 0.012) * (1.0 - identity)
    imag_off = noise_draw(second_key, (FREQ, NORB, NORB), 0.012) * (1.0 - identity)
    real_diag = jax.random.uniform(third_key, (FREQ, NORB), jnp.float32, -0.3, 0.3)
    damping = jax.random.uniform(fourth_key, (FREQ, NORB), jnp.float32, -0.8, -0.4)
    real_part = real_off + real_diag[:, :, None] * identity
    imag_part = imag_off + damping[:, :, None] * identity
    return jnp.concatenate([real_part, imag_part], -1).astype(jnp.float32)


def draw_guess_factor(key, part):
    first_key, second_key, third_key = jax.random.split(key, 3)
    identity = jnp.eye(NORB, dtype=jnp.float32)
    real_off = noise_draw(first_key, (FREQ, NORB, NORB), 0.01) * (1.0 - identity)
    imag_part = noise_draw(second_key, (FREQ, NORB, NORB), 0.01)
    scales = jax.random.uniform(third_key, (FREQ, NORB), jnp.float32, 0.75, 1.25)
    real_part = real_off + scales[:, :, None] * identity
    return jnp.concatenate([real_part, imag_part], -1).astype(jnp.float32)


def draw_counts(key, part):
    positions = jnp.arange(FREQ, dtype=jnp.int32)
    extra = jax.random.randint(key, (FREQ,), 0, 4)
    lowest = (8 * positions < FREQ).astype(jnp.int32)
    bumped = ((extra == 0) & (positions < FREQ - 1)).astype(jnp.int32)
    return jnp.minimum(MAXIT, 1 + 2 * lowest + bumped).astype(jnp.int32)


def set_ends(drawn, stream_key, smallest, high):
    longest = drawn.shape.index(max(drawn.shape))
    spots = []
    for shift in (0, 1):
        where = [jax.random.randint(jax.random.fold_in(stream_key, axis), (), 0, length) for axis, length in enumerate(drawn.shape)]
        where[longest] = (where[longest] + shift) % drawn.shape[longest]
        spots.append(tuple(where))
    return drawn.at[spots[0]].set(smallest).at[spots[1]].set(high)


def setup_inputs(seed: int = 0) -> dict:
    keys = jax.random.split(jax.random.key(seed), 6)
    hamiltonian = draw_hamiltonian(jax.random.fold_in(keys[5], 71), 0)
    self_energy = draw_self_energy(jax.random.fold_in(keys[5], 71), 0)
    guess_factor = draw_guess_factor(jax.random.fold_in(keys[5], 71), 0)
    weights = set_ends(jax.random.randint(keys[3], (KPTS,), 1, 49), jax.random.fold_in(keys[3], 1), 1, 48).astype(jnp.int32)
    counts = draw_counts(jax.random.fold_in(keys[5], 71), 0)
    return dict(hamiltonian=hamiltonian, self_energy=self_energy, guess_factor=guess_factor, weights=weights, counts=counts)


chem_potential = 0.2


def blockify(right_side):
    order = right_side.shape[-1] // 2
    real_part = right_side[..., :order]
    imag_part = right_side[..., order:]
    upper_row = jnp.concatenate([real_part, imag_part], -1)
    lower_row = jnp.concatenate([-imag_part, real_part], -1)
    return jnp.concatenate([upper_row, lower_row], -2)


def complex_product(left_side, right_side):
    return jnp.einsum('...ij,...jl->...il', left_side, blockify(right_side), precision=lax.Precision.HIGHEST)


def build_matrix(kpoint_rows, sigma_rows, matsubara):
    orbitals = kpoint_rows.shape[1]
    identity = jnp.eye(orbitals, dtype=jnp.float32)
    real_shift = jnp.broadcast_to(chem_potential * identity, matsubara.shape + identity.shape)
    imag_shift = matsubara[:, None, None] * identity
    diagonal_shift = jnp.concatenate([real_shift, imag_shift], -1)
    return diagonal_shift[:, None] - kpoint_rows[None] - sigma_rows[:, None]


def start_guess(matrix, factor_rows):
    orbitals = matrix.shape[-2]
    diag_real = jnp.diagonal(matrix[..., :orbitals], axis1=-2, axis2=-1)
    diag_imag = jnp.diagonal(matrix[..., orbitals:], axis1=-2, axis2=-1)
    modulus = diag_real * diag_real + diag_imag * diag_imag
    recip_real = (diag_real / modulus)[..., None]
    recip_imag = (-diag_imag / modulus)[..., None]
    factor_real = factor_rows[..., :orbitals]
    factor_imag = factor_rows[..., orbitals:]
    guess_real = recip_real * factor_real - recip_imag * factor_imag
    guess_imag = recip_real * factor_imag + recip_imag * factor_real
    return jnp.concatenate([guess_real, guess_imag], -1)


def reference(hamiltonian, self_energy, guess_factor, weights, counts):
    orbitals = hamiltonian.shape[1]
    factors = weights.astype(jnp.float32)
    weight_total = jnp.sum(factors)
    identity = jnp.eye(orbitals, dtype=jnp.float32)
    doubled = jnp.concatenate([2.0 * identity, jnp.zeros_like(identity)], -1)

    def one_frequency(inputs):
        sigma_row, factor_row, step_count, freq_id = inputs
        matsubara = (2 * freq_id + 1).astype(jnp.float32)[None] * (math.pi / (2 * FREQ))
        matrix = build_matrix(hamiltonian, sigma_row[None], matsubara)
        initial = start_guess(matrix, factor_row[None, None])

        def newton_step(sweep, current):
            return complex_product(current, doubled - complex_product(matrix, current))

        final = lax.fori_loop(0, step_count, newton_step, initial)
        summed = jnp.einsum('k,fkij->fij', factors, final, precision=lax.Precision.HIGHEST)
        return summed[0] / weight_total

    greens = lax.map(one_frequency, (self_energy, guess_factor, counts, jnp.arange(FREQ, dtype=jnp.int32)))
    arranged = greens.reshape(FREQ, orbitals, 2, orbitals).transpose(1, 3, 2, 0)
    return arranged.reshape(orbitals * orbitals, 2 * FREQ)
```

```python
import functools
import math

import jax
import jax.numpy as jnp
from jax import lax
from jax.experimental import pallas as pl
from jax.experimental.pallas import tpu as pltpu
from jax.sharding import PartitionSpec as P

chem_potential = 0.2


def is_power_of_two(number):
    return number & (number - 1) == 0


def split_bf16(values):
    high = values.astype(jnp.bfloat16)
    low = (values - high.astype(jnp.float32)).astype(jnp.bfloat16)
    return high, low


def left_operand(values):
    high, low = split_bf16(values)
    return jnp.concatenate([high, low], -1)


def right_operand(values, swap_sign):
    width = values.shape[-1]
    block = jnp.concatenate([values, pltpu.roll(values, width // 2, 1) * swap_sign], 0)
    high, low = split_bf16(block)
    upper = jnp.concatenate([high, low], -1)
    lower = jnp.concatenate([high, jnp.zeros_like(low)], -1)
    return jnp.concatenate([upper, lower], 0)


def product(left, right):
    width = right.shape[-1] // 2
    both = jnp.dot(left, right, preferred_element_type=jnp.float32)
    return both[:, :width] + both[:, width:]


def green_kernel(
    sizes, weights_ref, counts_ref, *refs
):
    (z_devs, x_devs, c_devs, sub, k_local, group_devs, freq_total, orbitals, pieces) = sizes
    h_refs = refs[:pieces]
    sg_refs = refs[pieces:pieces + z_devs]
    out_ref = refs[pieces + z_devs]
    t_ref, hd_ref, wr_ref, g_ref, c_ref, r_ref, plane_ref = refs[pieces + z_devs + 1:]
    width = 2 * orbitals
    freqs = z_devs * sub
    k_total = pieces * k_local
    batch = math.gcd(k_total, 8)
    freq_pos = lax.axis_index("freq")
    group_pos = lax.axis_index("kgrp")
    z_pos, x_pos = freq_pos // x_devs, freq_pos % x_devs
    c_pos = group_pos % c_devs

    row = lax.broadcasted_iota(jnp.int32, (orbitals, width), 0)
    lane = lax.broadcasted_iota(jnp.int32, (orbitals, width), 1)
    in_left = lane < orbitals
    eye_left = (lane == row).astype(jnp.float32)
    eye_both = eye_left + (lane == row + orbitals).astype(jnp.float32)
    lane_row = lax.broadcasted_iota(jnp.int32, (1, width), 1)
    left_row = lane_row < orbitals
    swap_sign = jnp.where(left_row, -1.0, 1.0)

    def swap(values):
        return pltpu.roll(values, orbitals, 1)

    def block_of(step):
        if is_power_of_two(z_devs):
            return z_pos ^ step
        return (z_pos + z_devs - step) % z_devs

    def freq_of(step, member):
        return (block_of(step) * x_devs + x_pos) * (c_devs * sub) + c_pos * sub + member

    for step in range(z_devs):
        for member in range(sub):
            place = step * sub + member
            guess = sg_refs[step][1, member]
            sigma = sg_refs[step][0, member]
            freq_id = freq_of(step, member)
            matsubara = (2 * freq_id + 1).astype(jnp.float32) * (math.pi / (2 * freq_total))
            left = left_operand(guess)
            g_ref[pl.ds(place * orbitals, orbitals), :] = left
            shift = eye_left * chem_potential + (eye_both - eye_left) * matsubara
            c_ref[place] = product(left, right_operand(shift - sigma, swap_sign))

    for piece in range(pieces):
        x_flip, c_flip = piece // c_devs, piece % c_devs
        first_k = ((freq_pos ^ x_flip) * group_devs + (group_pos ^ c_flip)) * k_local

        def load_point(local, carry, piece=piece, first_k=first_k):
            place = piece * k_local + local
            matrix = h_refs[piece][local]
            t_ref[place] = product(g_ref[...], right_operand(matrix, swap_sign))
            diag = jnp.sum(matrix * eye_left, 0, keepdims=True)
            hd_ref[pl.ds(place, 1), :] = diag + swap(diag)
            weight = weights_ref[first_k + local].astype(jnp.float32)
            wr_ref[pl.ds(place, 1), :] = jnp.full((1, width), weight, jnp.float32)
            return carry

        lax.fori_loop(0, k_local, load_point, 0)

    def sum_frequency(place, count, sg_ref, member, freq_id, plane):
        matsubara = (2 * freq_id + 1).astype(jnp.float32) * (math.pi / (2 * freq_total))
        sigma_diag = jnp.sum(sg_ref[0, member] * eye_both, 0, keepdims=True)
        sigma_swap = swap(sigma_diag)
        real_base = chem_potential - jnp.where(left_row, sigma_diag, sigma_swap)
        imag = matsubara - jnp.where(left_row, sigma_swap, sigma_diag)
        constant = c_ref[place]
        r_ref[...] = jnp.zeros_like(r_ref)

        def accumulate(terms):
            def one_batch(step, carry):
                first = step * batch
                first_row = pl.multiple_of(first, batch)
                real = real_base - hd_ref[pl.ds(first_row, 8), :]
                modulus = real * real + imag * imag
                d_real = real / modulus
                d_swap = jnp.broadcast_to(imag, real.shape) / modulus * (-swap_sign)
                weight = wr_ref[pl.ds(first_row, 8), :]
                real_cols = jnp.transpose(d_real * weight)
                swap_cols = jnp.transpose(d_swap * weight)
                errors = []
                for item in range(batch):
                    mixed = constant - t_ref[first + item, pl.ds(place * orbitals, orbitals), :]
                    scaled = mixed * d_real[item:item + 1] + swap(mixed) * d_swap[item:item + 1]
                    errors.append(eye_left - scaled)
                total = r_ref[...]
                for item, series in enumerate(terms(errors)):
                    total = total + series * real_cols[:orbitals, item:item + 1]
                    turned = swap(series) * swap_sign
                    total = total + turned * swap_cols[orbitals:, item:item + 1]
                r_ref[...] = total
                return carry

            lax.fori_loop(0, k_total // batch, one_batch, 0)

        def one_step(errors):
            return [eye_left + error for error in errors]

        def cubic(errors):
            rights = [right_operand(error, swap_sign) for error in errors]
            squares = [product(left_operand(e), r) for e, r in zip(errors, rights)]
            cubes = [product(left_operand(s), r) for s, r in zip(squares, rights)]
            sums = [eye_left + e + s + c for e, s, c in zip(errors, squares, cubes)]
            return rights, cubes, sums

        def two_steps(errors):
            return cubic(errors)[2]

        def three_steps(errors):
            rights, cubes, sums = cubic(errors)
            fourths = [product(left_operand(c), r) for c, r in zip(cubes, rights)]
            lasts = [
                product(left_operand(s), right_operand(f, swap_sign)) for s, f in zip(sums, fourths)
            ]
            return [s + p for s, p in zip(sums, lasts)]

        @pl.when(count <= 1)
        def _():
            accumulate(one_step)

        @pl.when(count == 2)
        def _():
            accumulate(two_steps)

        @pl.when(count >= 3)
        def _():
            accumulate(three_steps)

        guess = sg_ref[1, member]
        r_ref[...] = product(left_operand(r_ref[...]), right_operand(guess, swap_sign))
        half = orbitals // 2
        even = r_ref[pl.ds(0, half, stride=2), :]
        odd = r_ref[pl.ds(1, half, stride=2), :]
        keep = in_left[:half]
        plane_ref[pl.ds(plane * half, half), :] = jnp.where(keep, even, swap(odd))
        plane_ref[pl.ds((freqs + plane) * half, half), :] = jnp.where(keep, swap(even), odd)

    for step in range(z_devs):
        for member in range(sub):
            freq_id = freq_of(step, member)
            sum_frequency(
                step * sub + member,
                counts_ref[freq_id],
                sg_refs[step],
                member,
                freq_id,
                block_of(step) * sub + member,
            )

    half = orbitals // 2
    for line in range(half):
        out_ref[line] = plane_ref[pl.ds(line, 2 * freqs, stride=half), :]


def final_kernel(sizes, weights_ref, parts_ref, out_ref):
    z_devs, x_devs, y_devs, c_devs, sub = sizes
    total = jnp.sum(weights_ref[...].astype(jnp.float32))
    shared = x_devs * c_devs
    for x_pos in range(x_devs):
        for c_pos in range(c_devs):
            gathered = None
            for z_pos in range(z_devs):
                for y_pos in range(y_devs):
                    source = ((z_pos * x_devs + x_pos) * y_devs + y_pos) * c_devs + c_pos
                    part = parts_ref[source]
                    gathered = part if gathered is None else gathered + part
            gathered = gathered / total
            place = x_pos * c_devs + c_pos
            if sub == 1:
                out_ref[pl.ds(place, 2 * z_devs, stride=shared), :] = gathered
            else:
                for group in range(2 * z_devs):
                    out_ref[pl.ds((group * shared + place) * sub, sub), :] = gathered[
                        group * sub:(group + 1) * sub
                    ]


def per_device(hamiltonian, self_energy, guess_factor, weights, counts):
    k_local, orbitals, width = hamiltonian.shape
    per_freq = self_energy.shape[0]
    freq_devs = lax.axis_size("freq")
    group_devs = lax.axis_size("kgrp")
    devices = freq_devs * group_devs
    freq_total = per_freq * freq_devs
    pair_block = orbitals * orbitals // devices
    x_devs = 2 if freq_devs % 2 == 0 else 1
    c_devs = 2 if group_devs % 2 == 0 and per_freq % 2 == 0 else 1
    z_devs = freq_devs // x_devs
    y_devs = group_devs // c_devs
    sub = per_freq // c_devs
    freqs = z_devs * sub
    c_pos = lax.axis_index("kgrp") % c_devs

    def core_flip(values):
        return lax.ppermute(values, "kgrp", [(i, i ^ 1) for i in range(group_devs)])

    def x_flip(values):
        return lax.ppermute(values, "freq", [(i, i ^ 1) for i in range(freq_devs)])

    def z_move(values, step):
        if is_power_of_two(z_devs):
            pairs = [(i, ((i // x_devs) ^ step) * x_devs + i % x_devs) for i in range(freq_devs)]
        else:
            pairs = [
                (i, (i // x_devs + step) % z_devs * x_devs + i % x_devs) for i in range(freq_devs)
            ]
        return lax.ppermute(values, "freq", pairs)

    own = jnp.stack([self_energy, guess_factor])
    own = lax.dynamic_slice_in_dim(own, c_pos * sub, sub, 1)
    sg_blocks = [own] + [z_move(own, step) for step in range(1, z_devs)]
    h_blocks = [hamiltonian]
    if x_devs == 2:
        h_blocks.append(x_flip(hamiltonian))
    if c_devs == 2:
        h_blocks = [piece for block in h_blocks for piece in (block, core_flip(block))]
    pieces = len(h_blocks)
    k_total = pieces * k_local
    k_rows = -(-k_total // 8) * 8

    vmem = pl.BlockSpec(memory_space=pltpu.VMEM)
    smem = pl.BlockSpec(memory_space=pltpu.SMEM)
    half = orbitals // 2
    partial_sums = pl.pallas_call(
        functools.partial(
            green_kernel,
            (z_devs, x_devs, c_devs, sub, k_local, group_devs, freq_total, orbitals, pieces),
        ),
        out_shape=jax.ShapeDtypeStruct((half, 2 * freqs, width), jnp.float32),
        in_specs=[smem, smem] + [vmem] * (pieces + z_devs),
        out_specs=vmem,
        scratch_shapes=[
            pltpu.VMEM((k_total, freqs * orbitals, width), jnp.float32),
            pltpu.VMEM((k_rows, width), jnp.float32),
            pltpu.VMEM((k_rows, width), jnp.float32),
            pltpu.VMEM((freqs * orbitals, 2 * width), jnp.bfloat16),
            pltpu.VMEM((freqs, orbitals, width), jnp.float32),
            pltpu.VMEM((orbitals, width), jnp.float32),
            pltpu.VMEM((2 * freqs * half, width), jnp.float32),
        ],
        compiler_params=pltpu.CompilerParams(vmem_limit_bytes=48 * 1024 * 1024),
        name="green",
    )(weights, counts, *h_blocks, *sg_blocks)

    share = width // pair_block
    outgoing = partial_sums.reshape(half, 2 * freqs, share, pair_block).transpose(0, 2, 1, 3)
    outgoing = outgoing.reshape(devices, 2 * freqs, pair_block)
    arrived = lax.all_to_all(outgoing, ("freq", "kgrp"), 0, 0, tiled=True)
    result = pl.pallas_call(
        functools.partial(final_kernel, (z_devs, x_devs, y_devs, c_devs, sub)),
        out_shape=jax.ShapeDtypeStruct((2 * freq_total, pair_block), jnp.float32),
        in_specs=[vmem, vmem],
        out_specs=vmem,
        name="collect",
    )(weights.reshape(1, -1), arrived)
    return result.T


def solution(mesh):
    return jax.shard_map(
        per_device,
        mesh=mesh,
        in_specs=(
            P(("freq", "kgrp"), None, None),
            P("freq", None, None),
            P("freq", None, None),
            P(),
            P(),
        ),
        out_specs=P(("freq", "kgrp"), None),
        check_vma=False,
    )
```

```python
import functools
import math

import jax
import jax.numpy as jnp
from jax import lax
from jax.experimental import pallas as pl
from jax.experimental.pallas import tpu as pltpu
from jax.sharding import PartitionSpec as P

chem_potential = 0.2
BATCH = 8
LOAD_BATCH = 8


def is_power_of_two(number):
    return number & (number - 1) == 0


def split_bf16(values):
    high = values.astype(jnp.bfloat16)
    low = (values - high.astype(jnp.float32)).astype(jnp.bfloat16)
    return high, low


def left_operand(values):
    high, low = split_bf16(values)
    return jnp.concatenate([high, low], -1)


def right_operand(values, swap_sign):
    width = values.shape[-1]
    block = jnp.concatenate([values, pltpu.roll(values, width // 2, 1) * swap_sign], 0)
    high, low = split_bf16(block)
    upper = jnp.concatenate([high, low], -1)
    lower = jnp.concatenate([high, jnp.zeros_like(low)], -1)
    return jnp.concatenate([upper, lower], 0)


def product(left, right):
    width = right.shape[-1] // 2
    both = jnp.dot(left, right, preferred_element_type=jnp.float32)
    return both[:, :width] + both[:, width:]


def green_kernel(sizes, first, weights_ref, counts_ref, *refs):
    (z_devs, x_devs, c_devs, sub, k_local, group_devs, freq_total, orbitals, flips) = sizes
    pieces = len(flips)
    width = 2 * orbitals
    half = orbitals // 2
    freqs = z_devs * sub
    k_total = pieces * k_local
    freq_pos = lax.axis_index("freq")
    group_pos = lax.axis_index("kgrp")
    z_pos, x_pos = freq_pos // x_devs, freq_pos % x_devs
    c_pos = group_pos % c_devs

    h_refs, refs = refs[:pieces], refs[pieces:]
    if first:
        sg_refs, refs = refs[:z_devs], refs[z_devs:]
        (sum_ref, left_ref, right_ref, shift_ref, rows_ref), refs = refs[:5], refs[5:]
        t_ref, hd_ref, wr_ref = refs
    else:
        (old_ref, left_ref, right_ref, shift_ref, rows_ref), refs = refs[:5], refs[5:]
        out_ref, t_ref, hd_ref, wr_ref, r_ref, plane_ref = refs

    row = lax.broadcasted_iota(jnp.int32, (orbitals, width), 0)
    lane = lax.broadcasted_iota(jnp.int32, (orbitals, width), 1)
    eye_left = (lane == row).astype(jnp.float32)
    eye_both = eye_left + (lane == row + orbitals).astype(jnp.float32)
    lane_row = lax.broadcasted_iota(jnp.int32, (1, width), 1)
    left_row = lane_row < orbitals
    swap_sign = jnp.where(left_row, -1.0, 1.0)

    def swap(values):
        return pltpu.roll(values, orbitals, 1)

    def block_of(step):
        if is_power_of_two(z_devs):
            return z_pos ^ step
        return (z_pos + z_devs - step) % z_devs

    def freq_of(place):
        step, member = place // sub, place % sub
        return (block_of(step) * x_devs + x_pos) * (c_devs * sub) + c_pos * sub + member

    if first:
        for place in range(freqs):
            step, member = place // sub, place % sub
            sigma = sg_refs[step][0, member]
            guess = sg_refs[step][1, member]
            matsubara = (2 * freq_of(place) + 1).astype(jnp.float32) * (math.pi / (2 * freq_total))
            left = left_operand(guess)
            left_ref[pl.ds(place * orbitals, orbitals), :] = left
            right_ref[place] = right_operand(guess, swap_sign)
            energy = eye_left * chem_potential + (eye_both - eye_left) * matsubara
            shift_ref[place] = product(left, right_operand(energy - sigma, swap_sign))
            sigma_diag = jnp.sum(sigma * eye_both, 0, keepdims=True)
            sigma_swap = swap(sigma_diag)
            rows_ref[place, pl.ds(0, 1), :] = chem_potential - jnp.where(
                left_row, sigma_diag, sigma_swap
            )
            rows_ref[place, pl.ds(1, 1), :] = matsubara - jnp.where(left_row, sigma_swap, sigma_diag)

    def load_points(piece, locals_):
        x_flip, c_flip = flips[piece]
        first_k = ((freq_pos ^ x_flip) * group_devs + (group_pos ^ c_flip)) * k_local
        rights = []
        for local in locals_:
            place = piece * k_local + local
            matrix = h_refs[piece][local]
            rights.append(right_operand(matrix, swap_sign))
            diag = jnp.sum(matrix * eye_left, 0, keepdims=True)
            hd_ref[pl.ds(place, 1), :] = diag + swap(diag)
            weight = weights_ref[first_k + local].astype(jnp.float32)
            wr_ref[pl.ds(place, 1), :] = jnp.full((1, width), weight, jnp.float32)
        for local, right in zip(locals_, rights):
            t_ref[piece * k_local + local] = product(left_ref[...], right)

    for piece in range(pieces):
        for start in range(0, k_local, LOAD_BATCH):
            load_points(piece, range(start, min(start + LOAD_BATCH, k_local)))

    def one_frequency(place, carry):
        real_base = rows_ref[place, pl.ds(0, 1), :]
        imag = rows_ref[place, pl.ds(1, 1), :]
        constant = shift_ref[place]
        count = counts_ref[freq_of(place)]
        real = real_base - hd_ref[...]
        modulus = real * real + imag * imag
        d_real = real / modulus
        d_swap = jnp.broadcast_to(imag, real.shape) / modulus * (-swap_sign)
        real_cols = jnp.transpose(d_real * wr_ref[...])
        swap_cols = jnp.transpose(d_swap * wr_ref[...])
        offset = pl.multiple_of(place * orbitals, orbitals)

        def accumulate(terms):
            total = jnp.zeros((orbitals, width), jnp.float32) if first else old_ref[place]
            for begin in range(0, k_total, BATCH):
                items = range(begin, min(begin + BATCH, k_total))
                errors = []
                for item in items:
                    mixed = constant - t_ref[item, pl.ds(offset, orbitals), :]
                    scaled = mixed * d_real[item:item + 1] + swap(mixed) * d_swap[item:item + 1]
                    errors.append(eye_left - scaled)
                for item, series in zip(items, terms(errors)):
                    total = total + series * real_cols[:orbitals, item:item + 1]
                    turned = swap(series) * swap_sign
                    total = total + turned * swap_cols[orbitals:, item:item + 1]
            if first:
                sum_ref[place] = total
            else:
                r_ref[...] = product(left_operand(total), right_ref[place])

        def one_step(errors):
            return [eye_left + error for error in errors]

        def two_steps(errors):
            rights = [right_operand(e, swap_sign) for e in errors]
            squares = [product(left_operand(e), r) for e, r in zip(errors, rights)]
            cubes = [product(left_operand(s), r) for s, r in zip(squares, rights)]
            return [eye_left + e + s + c for e, s, c in zip(errors, squares, cubes)]

        def three_steps(errors):
            rights = [right_operand(e, swap_sign) for e in errors]
            squares = [product(left_operand(e), r) for e, r in zip(errors, rights)]
            starts = [eye_left + e for e in errors]
            pairs = [jnp.concatenate([a, s], 0) for a, s in zip(starts, squares)]
            both = [
                product(left_operand(p), right_operand(s, swap_sign)) for p, s in zip(pairs, squares)
            ]
            sums = [a + b[:orbitals] for a, b in zip(starts, both)]
            lasts = [
                product(left_operand(s), right_operand(b[orbitals:], swap_sign))
                for s, b in zip(sums, both)
            ]
            return [s + p for s, p in zip(sums, lasts)]

        @pl.when(count <= 1)
        def _():
            accumulate(one_step)

        @pl.when(count == 2)
        def _():
            accumulate(two_steps)

        @pl.when(count >= 3)
        def _():
            accumulate(three_steps)

        if not first:
            even = r_ref[pl.ds(0, half, stride=2), :]
            odd = r_ref[pl.ds(1, half, stride=2), :]
            plane = block_of(place // sub) * sub + place % sub
            real_rows = pl.multiple_of(plane * half, half)
            imag_rows = pl.multiple_of((freqs + plane) * half, half)
            plane_ref[pl.ds(real_rows, half), :] = jnp.where(left_row, even, swap(odd))
            plane_ref[pl.ds(imag_rows, half), :] = jnp.where(left_row, swap(even), odd)
        return carry

    lax.fori_loop(0, freqs, one_frequency, 0)

    if not first:
        for line in range(half):
            out_ref[line] = plane_ref[pl.ds(line, 2 * freqs, stride=half), :]


def final_kernel(sizes, weights_ref, parts_ref, out_ref):
    z_devs, x_devs, y_devs, c_devs, sub = sizes
    total = jnp.sum(weights_ref[...].astype(jnp.float32))
    shared = x_devs * c_devs
    for x_pos in range(x_devs):
        for c_pos in range(c_devs):
            gathered = None
            for z_pos in range(z_devs):
                for y_pos in range(y_devs):
                    source = ((z_pos * x_devs + x_pos) * y_devs + y_pos) * c_devs + c_pos
                    part = parts_ref[source]
                    gathered = part if gathered is None else gathered + part
            gathered = gathered / total
            place = x_pos * c_devs + c_pos
            if sub == 1:
                out_ref[pl.ds(place, 2 * z_devs, stride=shared), :] = gathered
            else:
                for group in range(2 * z_devs):
                    out_ref[pl.ds((group * shared + place) * sub, sub), :] = gathered[
                        group * sub:(group + 1) * sub
                    ]


def per_device(hamiltonian, self_energy, guess_factor, weights, counts):
    k_local, orbitals, width = hamiltonian.shape
    per_freq = self_energy.shape[0]
    freq_devs = lax.axis_size("freq")
    group_devs = lax.axis_size("kgrp")
    devices = freq_devs * group_devs
    freq_total = per_freq * freq_devs
    pair_block = orbitals * orbitals // devices
    x_devs = 2 if freq_devs % 2 == 0 else 1
    c_devs = 2 if group_devs % 2 == 0 and per_freq % 2 == 0 else 1
    z_devs = freq_devs // x_devs
    y_devs = group_devs // c_devs
    sub = per_freq // c_devs
    freqs = z_devs * sub
    c_pos = lax.axis_index("kgrp") % c_devs

    def core_flip(values):
        return lax.ppermute(values, "kgrp", [(i, i ^ 1) for i in range(group_devs)])

    def x_flip(values):
        return lax.ppermute(values, "freq", [(i, i ^ 1) for i in range(freq_devs)])

    def z_move(values, step):
        if is_power_of_two(z_devs):
            pairs = [(i, ((i // x_devs) ^ step) * x_devs + i % x_devs) for i in range(freq_devs)]
        else:
            pairs = [
                (i, (i // x_devs + step) % z_devs * x_devs + i % x_devs) for i in range(freq_devs)
            ]
        return lax.ppermute(values, "freq", pairs)

    own = jnp.stack([self_energy, guess_factor])
    own = lax.dynamic_slice_in_dim(own, c_pos * sub, sub, 1)
    sg_blocks = [own] + [z_move(own, step) for step in range(1, z_devs)]
    near = [(hamiltonian, (0, 0))]
    far = []
    if x_devs == 2:
        crossing, _ = lax.optimization_barrier((hamiltonian, own))
        crossed = x_flip(crossing)
        crossed, sg_blocks = lax.optimization_barrier((crossed, sg_blocks))
        far.append((crossed, (1, 0)))
    if c_devs == 2:
        near += [(core_flip(block), (flip[0], 1)) for block, flip in near]
        far += [(core_flip(block), (flip[0], 1)) for block, flip in far]

    vmem = pl.BlockSpec(memory_space=pltpu.VMEM)
    smem = pl.BlockSpec(memory_space=pltpu.SMEM)
    half = orbitals // 2

    def run_kernel(first, points, extras, outputs, scratch, name):
        k_total = len(points) * k_local
        k_rows = -(-k_total // 8) * 8
        flips = tuple(flip for _, flip in points)
        sizes = (z_devs, x_devs, c_devs, sub, k_local, group_devs, freq_total, orbitals, flips)
        return pl.pallas_call(
            functools.partial(green_kernel, sizes, first),
            out_shape=outputs,
            in_specs=[smem, smem] + [vmem] * (len(points) + len(extras)),
            out_specs=jax.tree.map(lambda _: vmem, outputs),
            scratch_shapes=[
                pltpu.VMEM((k_total, freqs * orbitals, width), jnp.float32),
                pltpu.VMEM((k_rows, width), jnp.float32),
                pltpu.VMEM((k_rows, width), jnp.float32),
            ] + scratch,
            compiler_params=pltpu.CompilerParams(vmem_limit_bytes=40 * 1024 * 1024),
            name=name,
        )(weights, counts, *[block for block, _ in points], *extras)

    square = jax.ShapeDtypeStruct((freqs, orbitals, width), jnp.float32)
    shared = run_kernel(
        True,
        near,
        sg_blocks,
        (
            square,
            jax.ShapeDtypeStruct((freqs * orbitals, 2 * width), jnp.bfloat16),
            jax.ShapeDtypeStruct((freqs, 2 * width, 2 * width), jnp.bfloat16),
            square,
            jax.ShapeDtypeStruct((freqs, 8, width), jnp.float32),
        ),
        [],
        "near",
    )
    partial_sums = run_kernel(
        False,
        far,
        list(shared),
        jax.ShapeDtypeStruct((half, 2 * freqs, width), jnp.float32),
        [
            pltpu.VMEM((orbitals, width), jnp.float32),
            pltpu.VMEM((2 * freqs * half, width), jnp.float32),
        ],
        "far",
    )

    share = width // pair_block
    outgoing = partial_sums.reshape(half, 2 * freqs, share, pair_block).transpose(0, 2, 1, 3)
    outgoing = outgoing.reshape(devices, 2 * freqs, pair_block)
    arrived = lax.all_to_all(outgoing, ("freq", "kgrp"), 0, 0, tiled=True)
    result = pl.pallas_call(
        functools.partial(final_kernel, (z_devs, x_devs, y_devs, c_devs, sub)),
        out_shape=jax.ShapeDtypeStruct((2 * freq_total, pair_block), jnp.float32),
        in_specs=[vmem, vmem],
        out_specs=vmem,
        name="collect",
    )(weights.reshape(1, -1), arrived)
    return result.T


def solution(mesh):
    return jax.shard_map(
        per_device,
        mesh=mesh,
        in_specs=(
            P(("freq", "kgrp"), None, None),
            P("freq", None, None),
            P("freq", None, None),
            P(),
            P(),
        ),
        out_specs=P(("freq", "kgrp"), None),
        check_vma=False,
    )
```

```python
import functools
import math

import jax
import jax.numpy as jnp
from jax import lax
from jax.experimental import pallas as pl
from jax.experimental.pallas import tpu as pltpu
from jax.sharding import PartitionSpec as P


chem_potential = 0.2
BATCH = 8
COST = 400_000_000


def is_power_of_two(number):
    return number & (number - 1) == 0


def split_bf16(values):
    high = values.astype(jnp.bfloat16)
    low = (values - high.astype(jnp.float32)).astype(jnp.bfloat16)
    return high, low


def swap_halves(values):
    return pltpu.roll(values, values.shape[-1] // 2, 1)


def block_form(values, swap_sign):
    return jnp.concatenate([values, swap_halves(values) * swap_sign], 0)


def left_tile(high, low):
    return jnp.concatenate([high, low], -1)


def right_tile(high, low):
    upper = jnp.concatenate([high, low], -1)
    lower = jnp.concatenate([high, jnp.zeros_like(low)], -1)
    return jnp.concatenate([upper, lower], 0)


def add_halves(both):
    width = both.shape[-1] // 2
    return both[:, :width] + both[:, width:]


def product(left, right):
    return add_halves(jnp.dot(left, right, preferred_element_type=jnp.float32))


class Layout:
    def __init__(self, hamiltonian, self_energy):
        self.k_local, self.orbitals, self.width = hamiltonian.shape
        per_freq = self_energy.shape[0]
        self.freq_devs = lax.axis_size("freq")
        self.group_devs = lax.axis_size("kgrp")
        self.freq_total = per_freq * self.freq_devs
        self.x_devs = 2 if self.freq_devs % 2 == 0 else 1
        self.c_devs = 2 if self.group_devs % 2 == 0 and per_freq % 2 == 0 else 1
        self.z_devs = self.freq_devs // self.x_devs
        self.y_devs = self.group_devs // self.c_devs
        self.sub = per_freq // self.c_devs
        self.freqs = self.z_devs * self.sub

    def positions(self):
        freq_pos = lax.axis_index("freq")
        group_pos = lax.axis_index("kgrp")
        return freq_pos, group_pos, group_pos % self.c_devs

    def block_of(self, step):
        z_pos = lax.axis_index("freq") // self.x_devs
        if is_power_of_two(self.z_devs):
            return z_pos ^ step
        return (z_pos + self.z_devs - step) % self.z_devs

    def freq_of(self, place):
        freq_pos, _, c_pos = self.positions()
        block = self.block_of(place // self.sub) * self.x_devs + freq_pos % self.x_devs
        return block * (self.c_devs * self.sub) + c_pos * self.sub + place % self.sub

    def matsubara(self, place):
        return (2 * self.freq_of(place) + 1).astype(jnp.float32) * (math.pi / (2 * self.freq_total))

    def plane_of(self, place):
        return self.block_of(place // self.sub) * self.sub + place % self.sub


class Masks:
    def __init__(self, orbitals):
        width = 2 * orbitals
        row = lax.broadcasted_iota(jnp.int32, (orbitals, width), 0)
        lane = lax.broadcasted_iota(jnp.int32, (orbitals, width), 1)
        self.eye_left = (lane == row).astype(jnp.float32)
        self.eye_right = (lane == row + orbitals).astype(jnp.float32)
        self.eye_both = self.eye_left + self.eye_right
        self.eye_block = jnp.concatenate([self.eye_left, self.eye_right], 0)
        self.left_row = lax.broadcasted_iota(jnp.int32, (1, width), 1) < orbitals
        self.sign = jnp.where(self.left_row, -1.0, 1.0)


def prepare_frequency(plan, masks, place, sigma, guess, target, left_ref, right_ref, shift_ref, rows_ref):
    orbitals = plan.orbitals
    matsubara = plan.matsubara(place)
    high, low = split_bf16(block_form(guess, masks.sign))
    left = left_tile(high[:orbitals], low[:orbitals])
    left_ref[pl.ds(target * orbitals, orbitals), :] = left
    right_ref[target] = left_tile(high, low)
    energy = masks.eye_left * chem_potential + masks.eye_right * matsubara
    matrix = split_bf16(block_form(energy - sigma, masks.sign))
    shift_ref[target] = product(left, right_tile(*matrix))
    sigma_diag = jnp.sum(sigma * masks.eye_both, 0, keepdims=True)
    sigma_swap = swap_halves(sigma_diag)
    real = chem_potential - jnp.where(masks.left_row, sigma_diag, sigma_swap)
    imag = matsubara - jnp.where(masks.left_row, sigma_swap, sigma_diag)
    rows_ref[target, pl.ds(0, 1), :] = real
    rows_ref[target, pl.ds(1, 1), :] = imag


def diagonal_row(masks, matrix):
    diag = jnp.sum(matrix * masks.eye_left, 0, keepdims=True)
    return diag + swap_halves(diag)


def sum_points(plan, masks, rows, constant, load_t, diags, weights, total):
    orbitals = plan.orbitals
    real = rows[0:1] - diags
    imag = jnp.broadcast_to(rows[1:2], real.shape)
    modulus = real * real + imag * imag
    d_real = real / modulus
    d_imag = -imag / modulus
    d_start = jnp.where(masks.left_row, d_real, d_imag) * weights
    d_turned = d_imag * masks.sign
    d_signed = d_real * masks.sign

    def errors_of(items):
        errors = []
        for item in items:
            mixed = constant - load_t(item)
            turned = swap_halves(mixed)
            upper = mixed * d_real[item:item + 1] + turned * d_turned[item:item + 1]
            lower = turned * d_signed[item:item + 1] - mixed * d_imag[item:item + 1]
            errors.append(split_bf16(masks.eye_block - jnp.concatenate([upper, lower], 0)))
        return errors

    def advance(series, powers):
        next_series, next_powers = [], []
        for start, (high, low) in zip(series, powers):
            s_high, s_low = split_bf16(start)
            stacked = jnp.concatenate([left_tile(s_high, s_low), left_tile(high[:orbitals], low[:orbitals])], 0)
            both = product(stacked, right_tile(high, low))
            next_series.append(start + both[:orbitals])
            next_powers.append(split_bf16(block_form(both[orbitals:], masks.sign)))
        return next_series, next_powers

    def finish(total, series, powers):
        lefts = [left_tile(*split_bf16(start)) for start in series]
        rights = [right_tile(*power) for power in powers]
        for start in series:
            total = total + start
        return total + product(jnp.concatenate(lefts, 1), jnp.concatenate(rights, 0))

    def accumulate(advances, total):
        for begin in range(0, plan.k_total, BATCH):
            items = range(begin, min(begin + BATCH, plan.k_total))
            series = [masks.eye_both * d_start[item:item + 1] for item in items]
            powers = errors_of(items)
            for _ in range(advances):
                series, powers = advance(series, powers)
            total = finish(total, series, powers)
        return total

    return lambda advances: accumulate(advances, total)


def run_counts(count, accumulate, store):
    @pl.when(count <= 1)
    def _():
        store(accumulate(0))

    @pl.when(count == 2)
    def _():
        store(accumulate(1))

    @pl.when(count >= 3)
    def _():
        store(accumulate(2))


def first_kernel(plan, flips, weights_ref, counts_ref, sg_ref, *refs):
    k_local, orbitals = plan.k_local, plan.orbitals
    near = len(flips[0])
    h_refs, refs = refs[:near], refs[near:]
    sum_ref, left_ref, right_ref, shift_ref, rows_ref, hs_ref, hd_ref, wr_ref, t_ref = refs
    masks = Masks(orbitals)
    freq_pos, group_pos, _ = plan.positions()
    for place in range(plan.sub):
        prepare_frequency(
            plan, masks, place, sg_ref[0, place], sg_ref[1, place], place,
            left_ref, right_ref, shift_ref, rows_ref,
        )
    for group, members in enumerate(flips):
        for piece, (x_flip, c_flip) in enumerate(members):
            first_k = ((freq_pos ^ x_flip) * plan.group_devs + (group_pos ^ c_flip)) * k_local
            for local in range(k_local):
                weight = weights_ref[first_k + local].astype(jnp.float32)
                place = piece * k_local + local
                wr_ref[group, pl.ds(place, 1), :] = jnp.full((1, plan.width), weight, jnp.float32)
    for piece in range(near):
        for local in range(k_local):
            place = piece * k_local + local
            matrix = h_refs[piece][local]
            high, low = split_bf16(block_form(matrix, masks.sign))
            hs_ref[place] = left_tile(high, low)
            hd_ref[pl.ds(place, 1), :] = diagonal_row(masks, matrix)
            t_ref[place] = product(left_ref[...], right_tile(high, low))

    def one_frequency(place, carry):
        offset = pl.multiple_of(place * orbitals, orbitals)

        def store(total):
            sum_ref[place] = total

        accumulate = sum_points(
            plan, masks, rows_ref[place], shift_ref[place],
            lambda item: t_ref[item, pl.ds(offset, orbitals), :],
            hd_ref[...], wr_ref[0], jnp.zeros((orbitals, plan.width), jnp.float32),
        )
        run_counts(counts_ref[plan.freq_of(place)], accumulate, store)
        return carry

    lax.fori_loop(0, plan.sub, one_frequency, 0)


def near_kernel(plan, counts_ref, *refs):
    orbitals, width, sub = plan.orbitals, plan.width, plan.sub
    steps = plan.z_devs - 1
    sg_refs, refs = refs[:steps], refs[steps:]
    old_refs, refs = refs[:5], refs[5:]
    hs_ref, hd_ref, wr_ref = refs[:3]
    new_refs, (t_ref,) = refs[3:8], refs[8:]
    sum_ref, left_ref, right_ref, shift_ref, rows_ref = new_refs
    masks = Masks(orbitals)
    left_ref[pl.ds(0, sub * orbitals), :] = old_refs[1][...]
    for old_ref, new_ref in zip(old_refs, new_refs):
        if old_ref is not old_refs[1]:
            for place in range(sub):
                new_ref[place] = old_ref[place]
    for place in range(sub, plan.freqs):
        sg_ref = sg_refs[place // sub - 1]
        prepare_frequency(
            plan, masks, place, sg_ref[0, place % sub], sg_ref[1, place % sub], place,
            left_ref, right_ref, shift_ref, rows_ref,
        )
    lefts = left_ref[pl.ds(sub * orbitals, (plan.freqs - sub) * orbitals), :]
    for item in range(plan.k_total):
        tile = hs_ref[item]
        t_ref[item] = product(lefts, right_tile(tile[:, :width], tile[:, width:]))

    def one_frequency(place, carry):
        offset = pl.multiple_of((place - sub) * orbitals, orbitals)

        def store(total):
            sum_ref[place] = total

        accumulate = sum_points(
            plan, masks, rows_ref[place], shift_ref[place],
            lambda item: t_ref[item, pl.ds(offset, orbitals), :],
            hd_ref[...], wr_ref[0], jnp.zeros((orbitals, width), jnp.float32),
        )
        run_counts(counts_ref[plan.freq_of(place)], accumulate, store)
        return carry

    lax.fori_loop(sub, plan.freqs, one_frequency, 0)


def far_kernel(plan, group, pieces, counts_ref, *refs):
    k_local, orbitals, width, freqs = plan.k_local, plan.orbitals, plan.width, plan.freqs
    half = orbitals // 2
    h_refs, refs = refs[:pieces], refs[pieces:]
    old_ref, left_ref, right_ref, shift_ref, rows_ref, wr_ref = refs[:6]
    out_ref, t_ref, hd_ref, r_ref, plane_ref = refs[6:]
    masks = Masks(orbitals)
    for piece in range(pieces):
        for local in range(k_local):
            place = piece * k_local + local
            matrix = h_refs[piece][local]
            hd_ref[pl.ds(place, 1), :] = diagonal_row(masks, matrix)
            tile = right_tile(*split_bf16(block_form(matrix, masks.sign)))
            t_ref[place] = product(left_ref[...], tile)

    def one_frequency(place, carry):
        offset = pl.multiple_of(place * orbitals, orbitals)

        def store(total):
            tile = right_ref[place]
            right = right_tile(tile[:, :width], tile[:, width:])
            r_ref[...] = product(left_tile(*split_bf16(total)), right)

        if pieces:
            accumulate = sum_points(
                plan, masks, rows_ref[place], shift_ref[place],
                lambda item: t_ref[item, pl.ds(offset, orbitals), :],
                hd_ref[...], wr_ref[group], old_ref[place],
            )
            run_counts(counts_ref[plan.freq_of(place)], accumulate, store)
        else:
            store(old_ref[place])
        even = r_ref[pl.ds(0, half, stride=2), :]
        odd = r_ref[pl.ds(1, half, stride=2), :]
        plane = plan.plane_of(place)
        real_rows = pl.multiple_of(plane * half, half)
        imag_rows = pl.multiple_of((freqs + plane) * half, half)
        plane_ref[pl.ds(real_rows, half), :] = jnp.where(masks.left_row, even, swap_halves(odd))
        plane_ref[pl.ds(imag_rows, half), :] = jnp.where(masks.left_row, swap_halves(even), odd)
        return carry

    lax.fori_loop(0, freqs, one_frequency, 0)
    for line in range(half):
        out_ref[line] = plane_ref[pl.ds(line, 2 * freqs, stride=half), :]


def final_kernel(sizes, weights_ref, parts_ref, out_ref):
    z_devs, x_devs, y_devs, c_devs, sub = sizes
    total = jnp.sum(weights_ref[...].astype(jnp.float32))
    shared = x_devs * c_devs
    for x_pos in range(x_devs):
        for c_pos in range(c_devs):
            gathered = None
            for z_pos in range(z_devs):
                for y_pos in range(y_devs):
                    source = ((z_pos * x_devs + x_pos) * y_devs + y_pos) * c_devs + c_pos
                    part = parts_ref[source]
                    gathered = part if gathered is None else gathered + part
            gathered = gathered / total
            place = x_pos * c_devs + c_pos
            if sub == 1:
                out_ref[pl.ds(place, 2 * z_devs, stride=shared), :] = gathered
            else:
                for group in range(2 * z_devs):
                    out_ref[pl.ds((group * shared + place) * sub, sub), :] = gathered[
                        group * sub:(group + 1) * sub
                    ]


def local_green(hamiltonian, self_energy, guess_factor, weights, counts):
    plan = Layout(hamiltonian, self_energy)
    orbitals, width, sub, freqs = plan.orbitals, plan.width, plan.sub, plan.freqs
    x_devs, z_devs, k_local = plan.x_devs, plan.z_devs, plan.k_local
    devices = plan.freq_devs * plan.group_devs
    pair_block = orbitals * orbitals // devices
    half = orbitals // 2
    c_pos = plan.positions()[2]

    def core_flip(values):
        return lax.ppermute(values, "kgrp", [(i, i ^ 1) for i in range(plan.group_devs)])

    def x_flip(values):
        return lax.ppermute(values, "freq", [(i, i ^ 1) for i in range(plan.freq_devs)])

    def z_move(values, step):
        pairs = []
        for i in range(plan.freq_devs):
            z_pos, x_pos = i // x_devs, i % x_devs
            target = z_pos ^ step if is_power_of_two(z_devs) else (z_pos + step) % z_devs
            pairs.append((i, target * x_devs + x_pos))
        return lax.ppermute(values, "freq", pairs)

    own = jnp.stack([self_energy, guess_factor])
    own = lax.dynamic_slice_in_dim(own, c_pos * sub, sub, 1)
    others = [z_move(own, step) for step in range(1, z_devs)]
    near, near_flips, far, far_flips = [hamiltonian], [(0, 0)], [], []
    if plan.c_devs == 2:
        near.append(core_flip(hamiltonian))
        near_flips.append((0, 1))
    if x_devs == 2:
        crossing, _ = lax.optimization_barrier((hamiltonian, own))
        far.append(x_flip(crossing))
        far_flips.append((1, 0))
        if plan.c_devs == 2:
            far_flips.append((1, 1))
    flips = (tuple(near_flips), tuple(far_flips))
    plan.k_total = len(near) * k_local
    k_rows = -(-plan.k_total // 8) * 8

    vmem = pl.BlockSpec(memory_space=pltpu.VMEM)
    smem = pl.BlockSpec(memory_space=pltpu.SMEM)
    params = pltpu.CompilerParams(vmem_limit_bytes=40 * 1024 * 1024)

    estimate = pl.CostEstimate(flops=COST, bytes_accessed=1 << 20, transcendentals=0)

    def f32(*shape):
        return jax.ShapeDtypeStruct(shape, jnp.float32)

    def bf16(*shape):
        return jax.ShapeDtypeStruct(shape, jnp.bfloat16)

    def shared(places):
        return [
            f32(places, orbitals, width),
            bf16(places * orbitals, 2 * width),
            bf16(places, 2 * orbitals, 2 * width),
            f32(places, orbitals, width),
            f32(places, 8, width),
        ]

    outputs = shared(sub) + [
        bf16(plan.k_total, 2 * orbitals, 2 * width), f32(k_rows, width), f32(2, k_rows, width)
    ]
    lead = pl.pallas_call(
        functools.partial(first_kernel, plan, flips),
        out_shape=outputs,
        in_specs=[smem, smem] + [vmem] * (1 + len(near)),
        out_specs=[vmem] * len(outputs),
        scratch_shapes=[pltpu.VMEM((plan.k_total, sub * orbitals, width), jnp.float32)],
        compiler_params=params,
        cost_estimate=estimate,
        name="first",
    )
    *old, h_tiles, h_diags, w_rows = lead(weights, counts, own, *near)
    outputs = shared(freqs)
    shares = pl.pallas_call(
        functools.partial(near_kernel, plan),
        out_shape=outputs,
        in_specs=[smem] + [vmem] * (len(others) + len(old) + 3),
        out_specs=[vmem] * len(outputs),
        scratch_shapes=[pltpu.VMEM((plan.k_total, (freqs - sub) * orbitals, width), jnp.float32)],
        compiler_params=params,
        cost_estimate=estimate,
        name="near",
    )(counts, *others, *old, h_tiles, h_diags, w_rows)
    if far and plan.c_devs == 2:
        crossed, _ = lax.optimization_barrier((far[0], w_rows))
        far.append(core_flip(crossed))
    partial_sums = pl.pallas_call(
        functools.partial(far_kernel, plan, 1, len(far)),
        out_shape=f32(half, 2 * freqs, width),
        in_specs=[smem] + [vmem] * (len(far) + len(shares) + 1),
        out_specs=vmem,
        scratch_shapes=[
            pltpu.VMEM((plan.k_total, freqs * orbitals, width), jnp.float32),
            pltpu.VMEM((k_rows, width), jnp.float32),
            pltpu.VMEM((orbitals, width), jnp.float32),
            pltpu.VMEM((2 * freqs * half, width), jnp.float32),
        ],
        compiler_params=params,
        name="far",
    )(counts, *far, *shares, w_rows)

    share = width // pair_block
    outgoing = partial_sums.reshape(half, 2 * freqs, share, pair_block).transpose(0, 2, 1, 3)
    outgoing = outgoing.reshape(devices, 2 * freqs, pair_block)
    arrived = lax.all_to_all(outgoing, ("freq", "kgrp"), 0, 0, tiled=True)
    result = pl.pallas_call(
        functools.partial(final_kernel, (z_devs, x_devs, plan.y_devs, plan.c_devs, sub)),
        out_shape=f32(2 * plan.freq_total, pair_block),
        in_specs=[vmem, vmem],
        out_specs=vmem,
        name="collect",
    )(weights.reshape(1, -1), arrived)
    return result.T


def solution(mesh):
    return jax.shard_map(
        local_green,
        mesh=mesh,
        in_specs=(
            P(("freq", "kgrp"), None, None),
            P("freq", None, None),
            P("freq", None, None),
            P(),
            P(),
        ),
        out_specs=P(("freq", "kgrp"), None),
        check_vma=False,
    )
```

```python
import functools
import math

import jax
import jax.numpy as jnp
from jax import lax
from jax.experimental import pallas as pl
from jax.experimental.pallas import tpu as pltpu
from jax.sharding import PartitionSpec as P


chem_potential = 0.2
BATCH = 8
COST = 400_000_000


def is_power_of_two(number):
    return number & (number - 1) == 0


def split_bf16(values):
    high = values.astype(jnp.bfloat16)
    low = (values - high.astype(jnp.float32)).astype(jnp.bfloat16)
    return high, low


def swap_halves(values):
    return pltpu.roll(values, values.shape[-1] // 2, 1)


def block_form(values, swap_sign):
    return jnp.concatenate([values, swap_halves(values) * swap_sign], 0)


def left_tile(high, low):
    return jnp.concatenate([high, low], -1)


def right_tile(high, low):
    upper = jnp.concatenate([high, low], -1)
    lower = jnp.concatenate([high, jnp.zeros_like(low)], -1)
    return jnp.concatenate([upper, lower], 0)


def add_halves(both):
    width = both.shape[-1] // 2
    return both[:, :width] + both[:, width:]


def product(left, right):
    return add_halves(jnp.dot(left, right, preferred_element_type=jnp.float32))


class Layout:
    def __init__(self, hamiltonian, self_energy):
        self.k_local, self.orbitals, self.width = hamiltonian.shape
        per_freq = self_energy.shape[0]
        self.freq_devs = lax.axis_size("freq")
        self.group_devs = lax.axis_size("kgrp")
        self.freq_total = per_freq * self.freq_devs
        self.x_devs = 2 if self.freq_devs % 2 == 0 else 1
        self.c_devs = 2 if self.group_devs % 2 == 0 and per_freq % 2 == 0 else 1
        self.z_devs = self.freq_devs // self.x_devs
        self.y_devs = self.group_devs // self.c_devs
        self.sub = per_freq // self.c_devs
        self.freqs = self.z_devs * self.sub
        self.lead_steps = min(2, self.z_devs)
        self.lead = self.lead_steps * self.sub

    def positions(self):
        freq_pos = lax.axis_index("freq")
        group_pos = lax.axis_index("kgrp")
        return freq_pos, group_pos, group_pos % self.c_devs

    def block_of(self, step):
        z_pos = lax.axis_index("freq") // self.x_devs
        if is_power_of_two(self.z_devs):
            return z_pos ^ step
        return (z_pos + self.z_devs - step) % self.z_devs

    def freq_of(self, place):
        freq_pos, _, c_pos = self.positions()
        block = self.block_of(place // self.sub) * self.x_devs + freq_pos % self.x_devs
        return block * (self.c_devs * self.sub) + c_pos * self.sub + place % self.sub

    def matsubara(self, place):
        return (2 * self.freq_of(place) + 1).astype(jnp.float32) * (math.pi / (2 * self.freq_total))

    def plane_of(self, place):
        return self.block_of(place // self.sub) * self.sub + place % self.sub


class Masks:
    def __init__(self, orbitals):
        width = 2 * orbitals
        row = lax.broadcasted_iota(jnp.int32, (orbitals, width), 0)
        lane = lax.broadcasted_iota(jnp.int32, (orbitals, width), 1)
        self.eye_left = (lane == row).astype(jnp.float32)
        self.eye_right = (lane == row + orbitals).astype(jnp.float32)
        self.eye_both = self.eye_left + self.eye_right
        self.eye_block = jnp.concatenate([self.eye_left, self.eye_right], 0)
        self.left_row = lax.broadcasted_iota(jnp.int32, (1, width), 1) < orbitals
        self.sign = jnp.where(self.left_row, -1.0, 1.0)


def prepare_frequency(plan, masks, place, sigma, guess, target, left_ref, right_ref, shift_ref, rows_ref):
    orbitals = plan.orbitals
    matsubara = plan.matsubara(place)
    high, low = split_bf16(block_form(guess, masks.sign))
    left = left_tile(high[:orbitals], low[:orbitals])
    left_ref[pl.ds(target * orbitals, orbitals), :] = left
    right_ref[target] = left_tile(high, low)
    energy = masks.eye_left * chem_potential + masks.eye_right * matsubara
    matrix = split_bf16(block_form(energy - sigma, masks.sign))
    shift_ref[target] = product(left, right_tile(*matrix))
    sigma_diag = jnp.sum(sigma * masks.eye_both, 0, keepdims=True)
    sigma_swap = swap_halves(sigma_diag)
    real = chem_potential - jnp.where(masks.left_row, sigma_diag, sigma_swap)
    imag = matsubara - jnp.where(masks.left_row, sigma_swap, sigma_diag)
    rows_ref[target, pl.ds(0, 1), :] = real
    rows_ref[target, pl.ds(1, 1), :] = imag


def diagonal_row(masks, matrix):
    diag = jnp.sum(matrix * masks.eye_left, 0, keepdims=True)
    return diag + swap_halves(diag)


def sum_points(plan, masks, rows, constant, load_t, diags, weights, total):
    orbitals = plan.orbitals
    real = rows[0:1] - diags
    imag = jnp.broadcast_to(rows[1:2], real.shape)
    modulus = real * real + imag * imag
    d_real = real / modulus
    d_imag = -imag / modulus
    d_start = jnp.where(masks.left_row, d_real, d_imag) * weights
    d_turned = d_imag * masks.sign
    d_signed = d_real * masks.sign

    def errors_of(items):
        errors = []
        for item in items:
            mixed = constant - load_t(item)
            turned = swap_halves(mixed)
            upper = mixed * d_real[item:item + 1] + turned * d_turned[item:item + 1]
            lower = turned * d_signed[item:item + 1] - mixed * d_imag[item:item + 1]
            errors.append(split_bf16(masks.eye_block - jnp.concatenate([upper, lower], 0)))
        return errors

    def advance(series, powers):
        next_series, next_powers = [], []
        for start, (high, low) in zip(series, powers):
            s_high, s_low = split_bf16(start)
            stacked = jnp.concatenate([left_tile(s_high, s_low), left_tile(high[:orbitals], low[:orbitals])], 0)
            both = product(stacked, right_tile(high, low))
            next_series.append(start + both[:orbitals])
            next_powers.append(split_bf16(block_form(both[orbitals:], masks.sign)))
        return next_series, next_powers

    def finish(total, series, powers):
        lefts = [left_tile(*split_bf16(start)) for start in series]
        rights = [right_tile(*power) for power in powers]
        for start in series:
            total = total + start
        return total + product(jnp.concatenate(lefts, 1), jnp.concatenate(rights, 0))

    def accumulate(advances, total):
        for begin in range(0, plan.k_total, BATCH):
            items = range(begin, min(begin + BATCH, plan.k_total))
            series = [masks.eye_both * d_start[item:item + 1] for item in items]
            powers = errors_of(items)
            for _ in range(advances):
                series, powers = advance(series, powers)
            total = finish(total, series, powers)
        return total

    return lambda advances: accumulate(advances, total)


def run_counts(count, accumulate, store):
    @pl.when(count <= 1)
    def _():
        store(accumulate(0))

    @pl.when(count == 2)
    def _():
        store(accumulate(1))

    @pl.when(count >= 3)
    def _():
        store(accumulate(2))


def fetch(source_ref, target_ref, semaphore):
    copy = pltpu.make_async_copy(source_ref, target_ref, semaphore)
    copy.start()
    return copy


def first_kernel(plan, flips, weights_ref, counts_ref, own_ref, *refs):
    k_local, orbitals = plan.k_local, plan.orbitals
    sg_refs, refs = refs[:plan.lead_steps], refs[plan.lead_steps:]
    mates = len(flips[0]) - 1
    mate_refs, refs = refs[:mates], refs[mates:]
    sum_ref, left_ref, right_ref, shift_ref, rows_ref, hs_ref, hd_ref, wr_ref = refs[:8]
    t_ref, h_ref, weight_ref, count_ref, sems = refs[8:]
    masks = Masks(orbitals)
    own_copy = fetch(own_ref, h_ref, sems.at[0])
    weight_copy = fetch(weights_ref, weight_ref, sems.at[1])
    count_copy = fetch(counts_ref, count_ref, sems.at[2])
    freq_pos, group_pos, _ = plan.positions()
    for place in range(plan.lead):
        sg_ref = sg_refs[place // plan.sub]
        member = place % plan.sub
        prepare_frequency(
            plan, masks, place, sg_ref[0, member], sg_ref[1, member], place,
            left_ref, right_ref, shift_ref, rows_ref,
        )

    def load_piece(piece, source_ref):
        for local in range(k_local):
            place = piece * k_local + local
            matrix = source_ref[local]
            high, low = split_bf16(block_form(matrix, masks.sign))
            hs_ref[place] = left_tile(high, low)
            hd_ref[pl.ds(place, 1), :] = diagonal_row(masks, matrix)
            t_ref[place] = product(left_ref[...], right_tile(high, low))

    for piece, mate_ref in enumerate(mate_refs):
        load_piece(piece + 1, mate_ref)
    own_copy.wait()
    load_piece(0, h_ref)
    weight_copy.wait()
    count_copy.wait()
    for group, members in enumerate(flips):
        for piece, (x_flip, c_flip) in enumerate(members):
            first_k = ((freq_pos ^ x_flip) * plan.group_devs + (group_pos ^ c_flip)) * k_local
            for local in range(k_local):
                weight = weight_ref[first_k + local].astype(jnp.float32)
                place = piece * k_local + local
                wr_ref[group, pl.ds(place, 1), :] = jnp.full((1, plan.width), weight, jnp.float32)

    def one_frequency(place, carry):
        offset = pl.multiple_of(place * orbitals, orbitals)

        def store(total):
            sum_ref[place] = total

        accumulate = sum_points(
            plan, masks, rows_ref[place], shift_ref[place],
            lambda item: t_ref[item, pl.ds(offset, orbitals), :],
            hd_ref[...], wr_ref[0], jnp.zeros((orbitals, plan.width), jnp.float32),
        )
        run_counts(count_ref[plan.freq_of(place)], accumulate, store)
        return carry

    lax.fori_loop(0, plan.lead, one_frequency, 0)


def near_kernel(plan, counts_ref, *refs):
    orbitals, width, sub, lead = plan.orbitals, plan.width, plan.sub, plan.lead
    steps = plan.z_devs - plan.lead_steps
    sg_refs, refs = refs[:steps], refs[steps:]
    old_refs, refs = refs[:5], refs[5:]
    hs_ref, hd_ref, wr_ref = refs[:3]
    new_refs, (t_ref, count_ref, sems) = refs[3:8], refs[8:]
    sum_ref, left_ref, right_ref, shift_ref, rows_ref = new_refs
    masks = Masks(orbitals)
    count_copy = fetch(counts_ref, count_ref, sems.at[0])
    for place in range(lead, plan.freqs):
        sg_ref = sg_refs[place // sub - plan.lead_steps]
        prepare_frequency(
            plan, masks, place, sg_ref[0, place % sub], sg_ref[1, place % sub], place,
            left_ref, right_ref, shift_ref, rows_ref,
        )
    lefts = left_ref[pl.ds(lead * orbitals, (plan.freqs - lead) * orbitals), :]
    for item in range(plan.k_total):
        tile = hs_ref[item]
        t_ref[item] = product(lefts, right_tile(tile[:, :width], tile[:, width:]))
    left_ref[pl.ds(0, lead * orbitals), :] = old_refs[1][...]
    for old_ref, new_ref in zip(old_refs, new_refs):
        if old_ref is not old_refs[1]:
            for place in range(lead):
                new_ref[place] = old_ref[place]
    count_copy.wait()

    def one_frequency(place, carry):
        offset = pl.multiple_of((place - lead) * orbitals, orbitals)

        def store(total):
            sum_ref[place] = total

        accumulate = sum_points(
            plan, masks, rows_ref[place], shift_ref[place],
            lambda item: t_ref[item, pl.ds(offset, orbitals), :],
            hd_ref[...], wr_ref[0], jnp.zeros((orbitals, width), jnp.float32),
        )
        run_counts(count_ref[plan.freq_of(place)], accumulate, store)
        return carry

    lax.fori_loop(lead, plan.freqs, one_frequency, 0)


def far_kernel(plan, group, pieces, counts_ref, *refs):
    k_local, orbitals, width, freqs = plan.k_local, plan.orbitals, plan.width, plan.freqs
    half = orbitals // 2
    h_refs, refs = refs[:pieces], refs[pieces:]
    old_ref, left_ref, right_ref, shift_ref, rows_ref, wr_ref = refs[:6]
    out_ref, t_ref, hd_ref, r_ref, plane_ref, count_ref, sems = refs[6:]
    masks = Masks(orbitals)
    count_copy = fetch(counts_ref, count_ref, sems.at[0])
    for piece in range(pieces):
        for local in range(k_local):
            place = piece * k_local + local
            matrix = h_refs[piece][local]
            hd_ref[pl.ds(place, 1), :] = diagonal_row(masks, matrix)
            tile = right_tile(*split_bf16(block_form(matrix, masks.sign)))
            t_ref[place] = product(left_ref[...], tile)
    count_copy.wait()

    def one_frequency(place, carry):
        offset = pl.multiple_of(place * orbitals, orbitals)

        def store(total):
            r_ref[place] = total

        accumulate = sum_points(
            plan, masks, rows_ref[place], shift_ref[place],
            lambda item: t_ref[item, pl.ds(offset, orbitals), :],
            hd_ref[...], wr_ref[group], old_ref[place],
        )
        run_counts(count_ref[plan.freq_of(place)], accumulate, store)
        return carry

    if pieces:
        lax.fori_loop(0, freqs, one_frequency, 0)
    totals = r_ref if pieces else old_ref
    greens = []
    for place in range(freqs):
        tile = right_ref[place]
        right = right_tile(tile[:, :width], tile[:, width:])
        greens.append(product(left_tile(*split_bf16(totals[place])), right))
    for place, green in enumerate(greens):
        r_ref[place] = green
    for place in range(freqs):
        even = r_ref[place, pl.ds(0, half, stride=2), :]
        odd = r_ref[place, pl.ds(1, half, stride=2), :]
        plane = plan.plane_of(place)
        real_rows = pl.multiple_of(plane * half, half)
        imag_rows = pl.multiple_of((freqs + plane) * half, half)
        plane_ref[pl.ds(real_rows, half), :] = jnp.where(masks.left_row, even, swap_halves(odd))
        plane_ref[pl.ds(imag_rows, half), :] = jnp.where(masks.left_row, swap_halves(even), odd)
    for line in range(half):
        out_ref[line] = plane_ref[pl.ds(line, 2 * freqs, stride=half), :]


def final_kernel(sizes, weights_ref, parts_ref, out_ref):
    z_devs, x_devs, y_devs, c_devs, sub = sizes
    total = jnp.sum(weights_ref[...].astype(jnp.float32))
    shared = x_devs * c_devs
    for x_pos in range(x_devs):
        for c_pos in range(c_devs):
            gathered = None
            for z_pos in range(z_devs):
                for y_pos in range(y_devs):
                    source = ((z_pos * x_devs + x_pos) * y_devs + y_pos) * c_devs + c_pos
                    part = parts_ref[source]
                    gathered = part if gathered is None else gathered + part
            gathered = gathered / total
            place = x_pos * c_devs + c_pos
            if sub == 1:
                out_ref[pl.ds(place, 2 * z_devs, stride=shared), :] = gathered
            else:
                for group in range(2 * z_devs):
                    out_ref[pl.ds((group * shared + place) * sub, sub), :] = gathered[
                        group * sub:(group + 1) * sub
                    ]


def local_green(hamiltonian, self_energy, guess_factor, weights, counts):
    plan = Layout(hamiltonian, self_energy)
    orbitals, width, sub, freqs = plan.orbitals, plan.width, plan.sub, plan.freqs
    x_devs, z_devs, k_local = plan.x_devs, plan.z_devs, plan.k_local
    devices = plan.freq_devs * plan.group_devs
    pair_block = orbitals * orbitals // devices
    half = orbitals // 2
    c_pos = plan.positions()[2]

    def core_flip(values):
        return lax.ppermute(values, "kgrp", [(i, i ^ 1) for i in range(plan.group_devs)])

    def x_flip(values):
        return lax.ppermute(values, "freq", [(i, i ^ 1) for i in range(plan.freq_devs)])

    def z_move(values, step):
        pairs = []
        for i in range(plan.freq_devs):
            z_pos, x_pos = i // x_devs, i % x_devs
            target = z_pos ^ step if is_power_of_two(z_devs) else (z_pos + step) % z_devs
            pairs.append((i, target * x_devs + x_pos))
        return lax.ppermute(values, "freq", pairs)

    own = jnp.stack([self_energy, guess_factor])
    own = lax.dynamic_slice_in_dim(own, c_pos * sub, sub, 1)
    others = [z_move(own, step) for step in reversed(range(plan.lead_steps, z_devs))][::-1]
    leading = [own] + [z_move(own, step) for step in range(1, plan.lead_steps)]
    near, near_flips, far, far_flips = [hamiltonian], [(0, 0)], [], []
    if plan.c_devs == 2:
        near.append(core_flip(hamiltonian))
        near_flips.append((0, 1))
    if x_devs == 2:
        crossing, _ = lax.optimization_barrier((hamiltonian, own))
        far.append(x_flip(crossing))
        far_flips.append((1, 0))
        if plan.c_devs == 2:
            far_flips.append((1, 1))
    flips = (tuple(near_flips), tuple(far_flips))
    plan.k_total = len(near) * k_local
    k_rows = -(-plan.k_total // 8) * 8

    vmem = pl.BlockSpec(memory_space=pltpu.VMEM)
    outside = pl.BlockSpec(memory_space=pltpu.HBM)

    def in_hbm(values):
        return pltpu.with_memory_space_constraint(values, pltpu.HBM)

    count_scratch = pltpu.SMEM(counts.shape, counts.dtype)
    far_counts = in_hbm(counts)
    params = pltpu.CompilerParams(vmem_limit_bytes=40 * 1024 * 1024)

    estimate = pl.CostEstimate(flops=COST, bytes_accessed=1 << 20, transcendentals=0)

    def f32(*shape):
        return jax.ShapeDtypeStruct(shape, jnp.float32)

    def bf16(*shape):
        return jax.ShapeDtypeStruct(shape, jnp.bfloat16)

    def shared(places):
        return [
            f32(places, orbitals, width),
            bf16(places * orbitals, 2 * width),
            bf16(places, 2 * orbitals, 2 * width),
            f32(places, orbitals, width),
            f32(places, 8, width),
        ]

    outputs = shared(plan.lead) + [
        bf16(plan.k_total, 2 * orbitals, 2 * width), f32(k_rows, width), f32(2, k_rows, width)
    ]
    lead = pl.pallas_call(
        functools.partial(first_kernel, plan, flips),
        out_shape=outputs,
        in_specs=[outside] * 3 + [vmem] * (len(leading) + len(near) - 1),
        out_specs=[vmem] * len(outputs),
        scratch_shapes=[
            pltpu.VMEM((plan.k_total, plan.lead * orbitals, width), jnp.float32),
            pltpu.VMEM((k_local, orbitals, width), jnp.float32),
            pltpu.SMEM(weights.shape, weights.dtype),
            count_scratch,
            pltpu.SemaphoreType.DMA((3,)),
        ],
        compiler_params=params,
        cost_estimate=estimate,
        name="first",
    )
    *old, h_tiles, h_diags, w_rows = lead(
        in_hbm(weights), far_counts, in_hbm(hamiltonian), *leading, *near[1:]
    )
    outputs = shared(freqs)
    shares = pl.pallas_call(
        functools.partial(near_kernel, plan),
        out_shape=outputs,
        in_specs=[outside] + [vmem] * (len(others) + len(old) + 3),
        out_specs=[vmem] * len(outputs),
        scratch_shapes=[
            pltpu.VMEM((plan.k_total, (freqs - plan.lead) * orbitals, width), jnp.float32),
            count_scratch,
            pltpu.SemaphoreType.DMA((1,)),
        ],
        compiler_params=params,
        cost_estimate=estimate,
        name="near",
    )(far_counts, *others, *old, h_tiles, h_diags, w_rows)
    if far and plan.c_devs == 2:
        crossed, _ = lax.optimization_barrier((far[0], w_rows))
        far.append(core_flip(crossed))
    partial_sums = pl.pallas_call(
        functools.partial(far_kernel, plan, 1, len(far)),
        out_shape=f32(half, 2 * freqs, width),
        in_specs=[outside] + [vmem] * (len(far) + len(shares) + 1),
        out_specs=vmem,
        scratch_shapes=[
            pltpu.VMEM((plan.k_total, freqs * orbitals, width), jnp.float32),
            pltpu.VMEM((k_rows, width), jnp.float32),
            pltpu.VMEM((freqs, orbitals, width), jnp.float32),
            pltpu.VMEM((2 * freqs * half, width), jnp.float32),
            count_scratch,
            pltpu.SemaphoreType.DMA((1,)),
        ],
        compiler_params=params,
        name="far",
    )(far_counts, *far, *shares, w_rows)

    share = width // pair_block
    outgoing = partial_sums.reshape(half, 2 * freqs, share, pair_block).transpose(0, 2, 1, 3)
    outgoing = outgoing.reshape(devices, 2 * freqs, pair_block)
    arrived = lax.all_to_all(outgoing, ("freq", "kgrp"), 0, 0, tiled=True)
    result = pl.pallas_call(
        functools.partial(final_kernel, (z_devs, x_devs, plan.y_devs, plan.c_devs, sub)),
        out_shape=f32(2 * plan.freq_total, pair_block),
        in_specs=[vmem, vmem],
        out_specs=vmem,
        name="collect",
    )(weights.reshape(1, -1), arrived)
    return result.T


def solution(mesh):
    return jax.shard_map(
        local_green,
        mesh=mesh,
        in_specs=(
            P(("freq", "kgrp"), None, None),
            P("freq", None, None),
            P("freq", None, None),
            P(),
            P(),
        ),
        out_specs=P(("freq", "kgrp"), None),
        check_vma=False,
    )
```

```python
import functools
import math

import jax
import jax.numpy as jnp
from jax import lax
from jax.experimental import pallas as pl
from jax.experimental.pallas import tpu as pltpu
from jax.sharding import PartitionSpec as P


chem_potential = 0.2
BATCH = 8
COST = 400_000_000


def is_power_of_two(number):
    return number & (number - 1) == 0


def split_bf16(values):
    high = values.astype(jnp.bfloat16)
    low = (values - high.astype(jnp.float32)).astype(jnp.bfloat16)
    return high, low


def swap_halves(values):
    return pltpu.roll(values, values.shape[-1] // 2, 1)


def block_form(values, swap_sign):
    return jnp.concatenate([values, swap_halves(values) * swap_sign], 0)


def split_block(values, swap_sign):
    high, low = split_bf16(values)
    sign = swap_sign.astype(jnp.bfloat16)
    return (
        jnp.concatenate([high, swap_halves(high) * sign], 0),
        jnp.concatenate([low, swap_halves(low) * sign], 0),
    )


def left_tile(high, low):
    return jnp.concatenate([high, low], -1)


def right_tile(high, low):
    upper = jnp.concatenate([high, low], -1)
    lower = jnp.concatenate([high, jnp.zeros_like(low)], -1)
    return jnp.concatenate([upper, lower], 0)


def add_halves(both):
    width = both.shape[-1] // 2
    return both[:, :width] + both[:, width:]


def product(left, right):
    return add_halves(jnp.dot(left, right, preferred_element_type=jnp.float32))


class Layout:
    def __init__(self, hamiltonian, self_energy):
        self.k_local, self.orbitals, self.width = hamiltonian.shape
        per_freq = self_energy.shape[0]
        self.freq_devs = lax.axis_size("freq")
        self.group_devs = lax.axis_size("kgrp")
        self.freq_total = per_freq * self.freq_devs
        self.x_devs = 2 if self.freq_devs % 2 == 0 else 1
        self.c_devs = 2 if self.group_devs % 2 == 0 and per_freq % 2 == 0 else 1
        self.z_devs = self.freq_devs // self.x_devs
        self.y_devs = self.group_devs // self.c_devs
        self.sub = per_freq // self.c_devs
        self.freqs = self.z_devs * self.sub
        self.lead_steps = min(2, self.z_devs)
        self.lead = self.lead_steps * self.sub

    def positions(self):
        freq_pos = lax.axis_index("freq")
        group_pos = lax.axis_index("kgrp")
        return freq_pos, group_pos, group_pos % self.c_devs

    def block_of(self, step):
        z_pos = lax.axis_index("freq") // self.x_devs
        if is_power_of_two(self.z_devs):
            return z_pos ^ step
        return (z_pos + self.z_devs - step) % self.z_devs

    def freq_of(self, place):
        freq_pos, _, c_pos = self.positions()
        block = self.block_of(place // self.sub) * self.x_devs + freq_pos % self.x_devs
        return block * (self.c_devs * self.sub) + c_pos * self.sub + place % self.sub

    def matsubara(self, place):
        return (2 * self.freq_of(place) + 1).astype(jnp.float32) * (math.pi / (2 * self.freq_total))

    def plane_of(self, place):
        return self.block_of(place // self.sub) * self.sub + place % self.sub


class Masks:
    def __init__(self, orbitals):
        width = 2 * orbitals
        row = lax.broadcasted_iota(jnp.int32, (orbitals, width), 0)
        lane = lax.broadcasted_iota(jnp.int32, (orbitals, width), 1)
        self.eye_left = (lane == row).astype(jnp.float32)
        self.eye_right = (lane == row + orbitals).astype(jnp.float32)
        self.eye_both = self.eye_left + self.eye_right
        self.eye_block = jnp.concatenate([self.eye_left, self.eye_right], 0)
        self.left_row = lax.broadcasted_iota(jnp.int32, (1, width), 1) < orbitals
        self.sign = jnp.where(self.left_row, -1.0, 1.0)


def prepare_frequency(plan, masks, place, sigma, guess, target, left_ref, right_ref, shift_ref, rows_ref):
    orbitals = plan.orbitals
    matsubara = plan.matsubara(place)
    high, low = split_bf16(block_form(guess, masks.sign))
    left = left_tile(high[:orbitals], low[:orbitals])
    left_ref[pl.ds(target * orbitals, orbitals), :] = left
    right_ref[target] = left_tile(high, low)
    energy = masks.eye_left * chem_potential + masks.eye_right * matsubara
    matrix = split_bf16(block_form(energy - sigma, masks.sign))
    shift_ref[target] = product(left, right_tile(*matrix))
    sigma_diag = jnp.sum(sigma * masks.eye_both, 0, keepdims=True)
    sigma_swap = swap_halves(sigma_diag)
    real = chem_potential - jnp.where(masks.left_row, sigma_diag, sigma_swap)
    imag = matsubara - jnp.where(masks.left_row, sigma_swap, sigma_diag)
    rows_ref[target, pl.ds(0, 1), :] = real
    rows_ref[target, pl.ds(1, 1), :] = imag


def diagonal_row(masks, matrix):
    diag = jnp.sum(matrix * masks.eye_left, 0, keepdims=True)
    return diag + swap_halves(diag)


def sum_points(plan, masks, rows, constant, load_t, diags, weights, total):
    orbitals = plan.orbitals
    real = rows[0:1] - diags
    imag = jnp.broadcast_to(rows[1:2], real.shape)
    modulus = real * real + imag * imag
    d_real = real / modulus
    d_imag = -imag / modulus
    d_start = jnp.where(masks.left_row, d_real, d_imag) * weights
    d_turned = d_imag * masks.sign
    d_signed = d_real * masks.sign

    def errors_of(items):
        errors = []
        for item in items:
            mixed = constant - load_t(item)
            turned = swap_halves(mixed)
            upper = mixed * d_real[item:item + 1] + turned * d_turned[item:item + 1]
            lower = turned * d_signed[item:item + 1] - mixed * d_imag[item:item + 1]
            errors.append(split_bf16(masks.eye_block - jnp.concatenate([upper, lower], 0)))
        return errors

    def advance(series, powers):
        next_series, next_powers = [], []
        for start, (high, low) in zip(series, powers):
            s_high, s_low = split_bf16(start)
            stacked = jnp.concatenate([left_tile(s_high, s_low), left_tile(high[:orbitals], low[:orbitals])], 0)
            both = product(stacked, right_tile(high, low))
            next_series.append(start + both[:orbitals])
            next_powers.append(split_block(both[orbitals:], masks.sign))
        return next_series, next_powers

    def finish(total, series, powers):
        lefts = [left_tile(*split_bf16(start)) for start in series]
        rights = [right_tile(*power) for power in powers]
        for start in series:
            total = total + start
        return total + product(jnp.concatenate(lefts, 1), jnp.concatenate(rights, 0))

    def accumulate(advances, total):
        for begin in range(0, plan.k_total, BATCH):
            items = range(begin, min(begin + BATCH, plan.k_total))
            series = [masks.eye_both * d_start[item:item + 1] for item in items]
            powers = errors_of(items)
            for _ in range(advances):
                series, powers = advance(series, powers)
            total = finish(total, series, powers)
        return total

    return lambda advances: accumulate(advances, total)


def run_counts(count, accumulate, store):
    @pl.when(count <= 1)
    def _():
        store(accumulate(0))

    @pl.when(count == 2)
    def _():
        store(accumulate(1))

    @pl.when(count >= 3)
    def _():
        store(accumulate(2))


def fetch(source_ref, target_ref, semaphore):
    copy = pltpu.make_async_copy(source_ref, target_ref, semaphore)
    copy.start()
    return copy


def first_kernel(plan, flips, weights_ref, counts_ref, own_ref, *refs):
    k_local, orbitals = plan.k_local, plan.orbitals
    sg_refs, refs = refs[:plan.lead_steps], refs[plan.lead_steps:]
    mates = len(flips[0]) - 1
    mate_refs, refs = refs[:mates], refs[mates:]
    sum_ref, left_ref, right_ref, shift_ref, rows_ref, hs_ref, hd_ref, wr_ref = refs[:8]
    t_ref, h_ref, weight_ref, count_ref, sems = refs[8:]
    masks = Masks(orbitals)
    own_copy = fetch(own_ref, h_ref, sems.at[0])
    weight_copy = fetch(weights_ref, weight_ref, sems.at[1])
    count_copy = fetch(counts_ref, count_ref, sems.at[2])
    freq_pos, group_pos, _ = plan.positions()
    for place in range(plan.lead):
        sg_ref = sg_refs[place // plan.sub]
        member = place % plan.sub
        prepare_frequency(
            plan, masks, place, sg_ref[0, member], sg_ref[1, member], place,
            left_ref, right_ref, shift_ref, rows_ref,
        )

    def load_piece(piece, source_ref):
        for local in range(k_local):
            place = piece * k_local + local
            matrix = source_ref[local]
            high, low = split_bf16(block_form(matrix, masks.sign))
            hs_ref[place] = left_tile(high, low)
            hd_ref[pl.ds(place, 1), :] = diagonal_row(masks, matrix)
            t_ref[place] = product(left_ref[...], right_tile(high, low))

    for piece, mate_ref in enumerate(mate_refs):
        load_piece(piece + 1, mate_ref)
    own_copy.wait()
    load_piece(0, h_ref)
    weight_copy.wait()
    count_copy.wait()
    for group, members in enumerate(flips):
        for piece, (x_flip, c_flip) in enumerate(members):
            first_k = ((freq_pos ^ x_flip) * plan.group_devs + (group_pos ^ c_flip)) * k_local
            for local in range(k_local):
                weight = weight_ref[first_k + local].astype(jnp.float32)
                place = piece * k_local + local
                wr_ref[group, pl.ds(place, 1), :] = jnp.full((1, plan.width), weight, jnp.float32)

    def one_frequency(place, carry):
        offset = pl.multiple_of(place * orbitals, orbitals)

        def store(total):
            sum_ref[place] = total

        accumulate = sum_points(
            plan, masks, rows_ref[place], shift_ref[place],
            lambda item: t_ref[item, pl.ds(offset, orbitals), :],
            hd_ref[...], wr_ref[0], jnp.zeros((orbitals, plan.width), jnp.float32),
        )
        run_counts(count_ref[plan.freq_of(place)], accumulate, store)
        return carry

    lax.fori_loop(0, plan.lead, one_frequency, 0)


def near_kernel(plan, counts_ref, *refs):
    orbitals, width, sub, lead = plan.orbitals, plan.width, plan.sub, plan.lead
    steps = plan.z_devs - plan.lead_steps
    sg_refs, refs = refs[:steps], refs[steps:]
    old_refs, refs = refs[:5], refs[5:]
    hs_ref, hd_ref, wr_ref = refs[:3]
    new_refs, (t_ref, count_ref, sems) = refs[3:8], refs[8:]
    sum_ref, left_ref, right_ref, shift_ref, rows_ref = new_refs
    masks = Masks(orbitals)
    count_copy = fetch(counts_ref, count_ref, sems.at[0])
    for place in range(lead, plan.freqs):
        sg_ref = sg_refs[place // sub - plan.lead_steps]
        prepare_frequency(
            plan, masks, place, sg_ref[0, place % sub], sg_ref[1, place % sub], place,
            left_ref, right_ref, shift_ref, rows_ref,
        )
    lefts = left_ref[pl.ds(lead * orbitals, (plan.freqs - lead) * orbitals), :]
    for item in range(plan.k_total):
        tile = hs_ref[item]
        t_ref[item] = product(lefts, right_tile(tile[:, :width], tile[:, width:]))
    left_ref[pl.ds(0, lead * orbitals), :] = old_refs[1][...]
    for old_ref, new_ref in zip(old_refs, new_refs):
        if old_ref is not old_refs[1]:
            for place in range(lead):
                new_ref[place] = old_ref[place]
    count_copy.wait()

    def one_frequency(place, carry):
        offset = pl.multiple_of((place - lead) * orbitals, orbitals)

        def store(total):
            sum_ref[place] = total

        accumulate = sum_points(
            plan, masks, rows_ref[place], shift_ref[place],
            lambda item: t_ref[item, pl.ds(offset, orbitals), :],
            hd_ref[...], wr_ref[0], jnp.zeros((orbitals, width), jnp.float32),
        )
        run_counts(count_ref[plan.freq_of(place)], accumulate, store)
        return carry

    lax.fori_loop(lead, plan.freqs, one_frequency, 0)


def far_kernel(plan, group, pieces, counts_ref, weights_ref, *refs):
    k_local, orbitals, width, freqs = plan.k_local, plan.orbitals, plan.width, plan.freqs
    half = orbitals // 2
    h_refs, refs = refs[:pieces], refs[pieces:]
    old_ref, left_ref, right_ref, shift_ref, rows_ref, wr_ref = refs[:6]
    out_ref, t_ref, hd_ref, r_ref, plane_ref, weight_ref, count_ref, sems = refs[6:]
    masks = Masks(orbitals)
    count_copy = fetch(counts_ref, count_ref, sems.at[0])
    weight_copy = fetch(weights_ref, weight_ref, sems.at[1])
    for piece in range(pieces):
        for local in range(k_local):
            place = piece * k_local + local
            matrix = h_refs[piece][local]
            hd_ref[pl.ds(place, 1), :] = diagonal_row(masks, matrix)
            tile = right_tile(*split_bf16(block_form(matrix, masks.sign)))
            t_ref[place] = product(left_ref[...], tile)
    count_copy.wait()

    def one_frequency(place, carry):
        offset = pl.multiple_of(place * orbitals, orbitals)

        def store(total):
            r_ref[place] = total

        accumulate = sum_points(
            plan, masks, rows_ref[place], shift_ref[place],
            lambda item: t_ref[item, pl.ds(offset, orbitals), :],
            hd_ref[...], wr_ref[group], old_ref[place],
        )
        run_counts(count_ref[plan.freq_of(place)], accumulate, store)
        return carry

    if pieces:
        lax.fori_loop(0, freqs, one_frequency, 0)
    totals = r_ref if pieces else old_ref
    greens = []
    for place in range(freqs):
        tile = right_ref[place]
        right = right_tile(tile[:, :width], tile[:, width:])
        greens.append(product(left_tile(*split_bf16(totals[place])), right))
    weight_copy.wait()
    norm = 1.0 / jnp.sum(weight_ref[...].astype(jnp.float32), keepdims=True)
    for place, green in enumerate(greens):
        r_ref[place] = green * norm
    for place in range(freqs):
        even = r_ref[place, pl.ds(0, half, stride=2), :]
        odd = r_ref[place, pl.ds(1, half, stride=2), :]
        plane = plan.plane_of(place)
        real_rows = pl.multiple_of(plane * half, half)
        imag_rows = pl.multiple_of((freqs + plane) * half, half)
        plane_ref[pl.ds(real_rows, half), :] = jnp.where(masks.left_row, even, swap_halves(odd))
        plane_ref[pl.ds(imag_rows, half), :] = jnp.where(masks.left_row, swap_halves(even), odd)
    for line in range(half):
        out_ref[line] = plane_ref[pl.ds(line, 2 * freqs, stride=half), :]


def local_green(hamiltonian, self_energy, guess_factor, weights, counts):
    plan = Layout(hamiltonian, self_energy)
    orbitals, width, sub, freqs = plan.orbitals, plan.width, plan.sub, plan.freqs
    x_devs, z_devs, k_local = plan.x_devs, plan.z_devs, plan.k_local
    devices = plan.freq_devs * plan.group_devs
    pair_block = orbitals * orbitals // devices
    half = orbitals // 2
    c_pos = plan.positions()[2]

    def core_flip(values):
        return lax.ppermute(values, "kgrp", [(i, i ^ 1) for i in range(plan.group_devs)])

    def x_flip(values):
        return lax.ppermute(values, "freq", [(i, i ^ 1) for i in range(plan.freq_devs)])

    def z_move(values, step):
        pairs = []
        for i in range(plan.freq_devs):
            z_pos, x_pos = i // x_devs, i % x_devs
            target = z_pos ^ step if is_power_of_two(z_devs) else (z_pos + step) % z_devs
            pairs.append((i, target * x_devs + x_pos))
        return lax.ppermute(values, "freq", pairs)

    own = jnp.stack([self_energy, guess_factor])
    own = lax.dynamic_slice_in_dim(own, c_pos * sub, sub, 1)
    others = [z_move(own, step) for step in reversed(range(plan.lead_steps, z_devs))][::-1]
    leading = [own] + [z_move(own, step) for step in range(1, plan.lead_steps)]
    near, near_flips, far, far_flips = [hamiltonian], [(0, 0)], [], []
    if plan.c_devs == 2:
        near.append(core_flip(hamiltonian))
        near_flips.append((0, 1))
    if x_devs == 2:
        crossing, _ = lax.optimization_barrier((hamiltonian, own))
        far.append(x_flip(crossing))
        far_flips.append((1, 0))
        if plan.c_devs == 2:
            far_flips.append((1, 1))
    flips = (tuple(near_flips), tuple(far_flips))
    plan.k_total = len(near) * k_local
    k_rows = -(-plan.k_total // 8) * 8

    vmem = pl.BlockSpec(memory_space=pltpu.VMEM)
    outside = pl.BlockSpec(memory_space=pltpu.HBM)

    def in_hbm(values):
        return pltpu.with_memory_space_constraint(values, pltpu.HBM)

    count_scratch = pltpu.SMEM(counts.shape, counts.dtype)
    far_counts = in_hbm(counts)
    params = pltpu.CompilerParams(vmem_limit_bytes=40 * 1024 * 1024)

    estimate = pl.CostEstimate(flops=COST, bytes_accessed=1 << 20, transcendentals=0)

    def f32(*shape):
        return jax.ShapeDtypeStruct(shape, jnp.float32)

    def bf16(*shape):
        return jax.ShapeDtypeStruct(shape, jnp.bfloat16)

    def shared(places):
        return [
            f32(places, orbitals, width),
            bf16(places * orbitals, 2 * width),
            bf16(places, 2 * orbitals, 2 * width),
            f32(places, orbitals, width),
            f32(places, 8, width),
        ]

    outputs = shared(plan.lead) + [
        bf16(plan.k_total, 2 * orbitals, 2 * width), f32(k_rows, width), f32(2, k_rows, width)
    ]
    lead = pl.pallas_call(
        functools.partial(first_kernel, plan, flips),
        out_shape=outputs,
        in_specs=[outside] * 3 + [vmem] * (len(leading) + len(near) - 1),
        out_specs=[vmem] * len(outputs),
        scratch_shapes=[
            pltpu.VMEM((plan.k_total, plan.lead * orbitals, width), jnp.float32),
            pltpu.VMEM((k_local, orbitals, width), jnp.float32),
            pltpu.SMEM(weights.shape, weights.dtype),
            count_scratch,
            pltpu.SemaphoreType.DMA((3,)),
        ],
        compiler_params=params,
        cost_estimate=estimate,
        name="first",
    )
    *old, h_tiles, h_diags, w_rows = lead(
        in_hbm(weights), far_counts, in_hbm(hamiltonian), *leading, *near[1:]
    )
    outputs = shared(freqs)
    shares = pl.pallas_call(
        functools.partial(near_kernel, plan),
        out_shape=outputs,
        in_specs=[outside] + [vmem] * (len(others) + len(old) + 3),
        out_specs=[vmem] * len(outputs),
        scratch_shapes=[
            pltpu.VMEM((plan.k_total, (freqs - plan.lead) * orbitals, width), jnp.float32),
            count_scratch,
            pltpu.SemaphoreType.DMA((1,)),
        ],
        compiler_params=pltpu.CompilerParams(vmem_limit_bytes=40 * 1024 * 1024),
        cost_estimate=estimate,
        name="near",
    )(far_counts, *others, *old, h_tiles, h_diags, w_rows)
    if far and plan.c_devs == 2:
        crossed, _ = lax.optimization_barrier((far[0], w_rows))
        far.append(core_flip(crossed))
    partial_sums = pl.pallas_call(
        functools.partial(far_kernel, plan, 1, len(far)),
        out_shape=f32(half, 2 * freqs, width),
        in_specs=[outside] * 2 + [vmem] * (len(far) + len(shares) + 1),
        out_specs=vmem,
        scratch_shapes=[
            pltpu.VMEM((plan.k_total, freqs * orbitals, width), jnp.float32),
            pltpu.VMEM((k_rows, width), jnp.float32),
            pltpu.VMEM((freqs, orbitals, width), jnp.float32),
            pltpu.VMEM((2 * freqs * half, width), jnp.float32),
            pltpu.VMEM((1, weights.size), weights.dtype),
            count_scratch,
            pltpu.SemaphoreType.DMA((2,)),
        ],
        compiler_params=params,
        name="far",
    )(far_counts, in_hbm(weights.reshape(1, -1)), *far, *shares, w_rows)

    share = width // pair_block
    outgoing = partial_sums.reshape(half, 2 * freqs, share, pair_block).transpose(0, 2, 1, 3)
    outgoing = outgoing.reshape(devices, 2 * freqs, pair_block)
    arrived = lax.all_to_all(outgoing, ("freq", "kgrp"), 0, 0, tiled=True)
    parts = arrived.reshape(z_devs, x_devs, plan.y_devs, plan.c_devs, 2, z_devs, sub, pair_block)
    result = jnp.sum(parts, (0, 2)).transpose(2, 3, 0, 1, 4, 5)
    return result.reshape(2 * plan.freq_total, pair_block).T


def solution(mesh):
    return jax.shard_map(
        local_green,
        mesh=mesh,
        in_specs=(
            P(("freq", "kgrp"), None, None),
            P("freq", None, None),
            P("freq", None, None),
            P(),
            P(),
        ),
        out_specs=P(("freq", "kgrp"), None),
        check_vma=False,
    )
```

```python
import functools
import math

import jax
import jax.numpy as jnp
from jax import lax
from jax.experimental import pallas as pl
from jax.experimental.pallas import tpu as pltpu
from jax.sharding import PartitionSpec as P


chem_potential = 0.2
BATCH = 8
COST = 400_000_000


def is_power_of_two(number):
    return number & (number - 1) == 0


def split_bf16(values):
    high = values.astype(jnp.bfloat16)
    low = (values - high.astype(jnp.float32)).astype(jnp.bfloat16)
    return high, low


def swap_halves(values):
    return pltpu.roll(values, values.shape[-1] // 2, 1)


def block_form(values, swap_sign):
    return jnp.concatenate([values, swap_halves(values) * swap_sign], 0)


def split_block(values, swap_sign):
    high, low = split_bf16(values)
    sign = swap_sign.astype(jnp.bfloat16)
    return (
        jnp.concatenate([high, swap_halves(high) * sign], 0),
        jnp.concatenate([low, swap_halves(low) * sign], 0),
    )


def left_tile(high, low):
    return jnp.concatenate([high, low], -1)


def right_tile(high, low):
    upper = jnp.concatenate([high, low], -1)
    lower = jnp.concatenate([high, jnp.zeros_like(low)], -1)
    return jnp.concatenate([upper, lower], 0)


def add_halves(both):
    width = both.shape[-1] // 2
    return both[:, :width] + both[:, width:]


def product(left, right):
    return add_halves(jnp.dot(left, right, preferred_element_type=jnp.float32))


class Layout:
    def __init__(self, hamiltonian, self_energy):
        self.k_local, self.orbitals, self.width = hamiltonian.shape
        per_freq = self_energy.shape[0]
        self.freq_devs = lax.axis_size("freq")
        self.group_devs = lax.axis_size("kgrp")
        self.freq_total = per_freq * self.freq_devs
        self.x_devs = 2 if self.freq_devs % 2 == 0 else 1
        self.c_devs = 2 if self.group_devs % 2 == 0 and per_freq % 2 == 0 else 1
        self.z_devs = self.freq_devs // self.x_devs
        self.y_devs = self.group_devs // self.c_devs
        self.sub = per_freq // self.c_devs
        self.freqs = self.z_devs * self.sub
        self.lead_steps = min(2, self.z_devs)
        self.lead = self.lead_steps * self.sub

    def positions(self):
        freq_pos = lax.axis_index("freq")
        group_pos = lax.axis_index("kgrp")
        return freq_pos, group_pos, group_pos % self.c_devs

    def block_of(self, step):
        z_pos = lax.axis_index("freq") // self.x_devs
        if is_power_of_two(self.z_devs):
            return z_pos ^ step
        return (z_pos + self.z_devs - step) % self.z_devs

    def freq_of(self, place):
        freq_pos, _, c_pos = self.positions()
        block = self.block_of(place // self.sub) * self.x_devs + freq_pos % self.x_devs
        return block * (self.c_devs * self.sub) + c_pos * self.sub + place % self.sub

    def matsubara(self, place):
        return (2 * self.freq_of(place) + 1).astype(jnp.float32) * (math.pi / (2 * self.freq_total))

    def plane_of(self, place):
        return self.block_of(place // self.sub) * self.sub + place % self.sub


class Masks:
    def __init__(self, orbitals):
        width = 2 * orbitals
        row = lax.broadcasted_iota(jnp.int32, (orbitals, width), 0)
        lane = lax.broadcasted_iota(jnp.int32, (orbitals, width), 1)
        self.eye_left = (lane == row).astype(jnp.float32)
        self.eye_right = (lane == row + orbitals).astype(jnp.float32)
        self.eye_both = self.eye_left + self.eye_right
        self.eye_block = jnp.concatenate([self.eye_left, self.eye_right], 0)
        self.left_row = lax.broadcasted_iota(jnp.int32, (1, width), 1) < orbitals
        self.sign = jnp.where(self.left_row, -1.0, 1.0)


def prepare_frequency(plan, masks, place, sigma, guess, target, left_ref, right_ref, shift_ref, rows_ref):
    orbitals = plan.orbitals
    matsubara = plan.matsubara(place)
    high, low = split_bf16(block_form(guess, masks.sign))
    left = left_tile(high[:orbitals], low[:orbitals])
    left_ref[pl.ds(target * orbitals, orbitals), :] = left
    right_ref[target] = left_tile(high, low)
    energy = masks.eye_left * chem_potential + masks.eye_right * matsubara
    matrix = split_bf16(block_form(energy - sigma, masks.sign))
    shift_ref[target] = product(left, right_tile(*matrix))
    sigma_diag = jnp.sum(sigma * masks.eye_both, 0, keepdims=True)
    sigma_swap = swap_halves(sigma_diag)
    real = chem_potential - jnp.where(masks.left_row, sigma_diag, sigma_swap)
    imag = matsubara - jnp.where(masks.left_row, sigma_swap, sigma_diag)
    rows_ref[target, pl.ds(0, 1), :] = real
    rows_ref[target, pl.ds(1, 1), :] = imag


def diagonal_row(masks, matrix):
    diag = jnp.sum(matrix * masks.eye_left, 0, keepdims=True)
    return diag + swap_halves(diag)


def sum_points(plan, masks, rows, constant, load_t, diags, weights, total):
    orbitals = plan.orbitals
    real = rows[0:1] - diags
    imag = jnp.broadcast_to(rows[1:2], real.shape)
    modulus = real * real + imag * imag
    d_real = real / modulus
    d_imag = -imag / modulus
    d_start = jnp.where(masks.left_row, d_real, d_imag) * weights
    d_high = d_start.astype(jnp.bfloat16).astype(jnp.float32)
    d_low = d_start - d_high
    d_turned = d_imag * masks.sign
    d_signed = d_real * masks.sign

    def errors_of(items):
        errors = []
        for item in items:
            mixed = constant - load_t(item)
            turned = swap_halves(mixed)
            upper = mixed * d_real[item:item + 1] + turned * d_turned[item:item + 1]
            lower = turned * d_signed[item:item + 1] - mixed * d_imag[item:item + 1]
            errors.append(split_bf16(masks.eye_block - jnp.concatenate([upper, lower], 0)))
        return errors

    def advance(series, lefts, powers):
        next_series, next_powers = [], []
        for start, left, (high, low) in zip(series, lefts, powers):
            stacked = jnp.concatenate([left, left_tile(high[:orbitals], low[:orbitals])], 0)
            both = product(stacked, right_tile(high, low))
            next_series.append(start + both[:orbitals])
            next_powers.append(split_block(both[orbitals:], masks.sign))
        return next_series, next_powers

    def finish(total, lefts, powers):
        rights = [right_tile(*power) for power in powers]
        return total + product(jnp.concatenate(lefts, 1), jnp.concatenate(rights, 0))

    def accumulate(advances, total):
        for begin in range(0, plan.k_total, BATCH):
            items = range(begin, min(begin + BATCH, plan.k_total))
            series = [masks.eye_both * d_start[item:item + 1] for item in items]
            powers = errors_of(items)
            lefts = [
                left_tile(
                    (masks.eye_both * d_high[item:item + 1]).astype(jnp.bfloat16),
                    (masks.eye_both * d_low[item:item + 1]).astype(jnp.bfloat16),
                )
                for item in items
            ]
            for _ in range(advances):
                series, powers = advance(series, lefts, powers)
                lefts = [left_tile(*split_bf16(start)) for start in series]
            if advances:
                for start in series:
                    total = total + start
            else:
                rows = d_start[begin:begin + len(items)]
                total = total + masks.eye_both * jnp.sum(rows, 0, keepdims=True)
            total = finish(total, lefts, powers)
        return total

    return lambda advances: accumulate(advances, total)


def run_counts(count, accumulate, store):
    @pl.when(count <= 1)
    def _():
        store(accumulate(0))

    @pl.when(count == 2)
    def _():
        store(accumulate(1))

    @pl.when(count >= 3)
    def _():
        store(accumulate(2))


def fetch(source_ref, target_ref, semaphore):
    copy = pltpu.make_async_copy(source_ref, target_ref, semaphore)
    copy.start()
    return copy


def first_kernel(plan, flips, weights_ref, counts_ref, own_ref, *refs):
    k_local, orbitals = plan.k_local, plan.orbitals
    sg_refs, refs = refs[:plan.lead_steps], refs[plan.lead_steps:]
    mates = len(flips[0]) - 1
    mate_refs, refs = refs[:mates], refs[mates:]
    sum_ref, left_ref, right_ref, shift_ref, rows_ref, hs_ref, hd_ref, wr_ref = refs[:8]
    t_ref, h_ref, weight_ref, count_ref, sems = refs[8:]
    masks = Masks(orbitals)
    own_copy = fetch(own_ref, h_ref, sems.at[0])
    weight_copy = fetch(weights_ref, weight_ref, sems.at[1])
    count_copy = fetch(counts_ref, count_ref, sems.at[2])
    freq_pos, group_pos, _ = plan.positions()
    for place in range(plan.lead):
        sg_ref = sg_refs[place // plan.sub]
        member = place % plan.sub
        prepare_frequency(
            plan, masks, place, sg_ref[0, member], sg_ref[1, member], place,
            left_ref, right_ref, shift_ref, rows_ref,
        )

    def load_piece(piece, source_ref):
        for local in range(k_local):
            place = piece * k_local + local
            matrix = source_ref[local]
            high, low = split_bf16(block_form(matrix, masks.sign))
            hs_ref[place] = left_tile(high, low)
            hd_ref[pl.ds(place, 1), :] = diagonal_row(masks, matrix)
            t_ref[place] = product(left_ref[...], right_tile(high, low))

    for piece, mate_ref in enumerate(mate_refs):
        load_piece(piece + 1, mate_ref)
    own_copy.wait()
    load_piece(0, h_ref)
    weight_copy.wait()
    count_copy.wait()
    for group, members in enumerate(flips):
        for piece, (x_flip, c_flip) in enumerate(members):
            first_k = ((freq_pos ^ x_flip) * plan.group_devs + (group_pos ^ c_flip)) * k_local
            for local in range(k_local):
                weight = weight_ref[first_k + local].astype(jnp.float32)
                place = piece * k_local + local
                wr_ref[group, pl.ds(place, 1), :] = jnp.full((1, plan.width), weight, jnp.float32)

    def one_frequency(place, carry):
        offset = pl.multiple_of(place * orbitals, orbitals)

        def store(total):
            sum_ref[place] = total

        accumulate = sum_points(
            plan, masks, rows_ref[place], shift_ref[place],
            lambda item: t_ref[item, pl.ds(offset, orbitals), :],
            hd_ref[...], wr_ref[0], jnp.zeros((orbitals, plan.width), jnp.float32),
        )
        run_counts(count_ref[plan.freq_of(place)], accumulate, store)
        return carry

    lax.fori_loop(0, plan.lead, one_frequency, 0)


def near_kernel(plan, counts_ref, *refs):
    orbitals, width, sub, lead = plan.orbitals, plan.width, plan.sub, plan.lead
    steps = plan.z_devs - plan.lead_steps
    sg_refs, refs = refs[:steps], refs[steps:]
    old_refs, refs = refs[:5], refs[5:]
    hs_ref, hd_ref, wr_ref = refs[:3]
    new_refs, (t_ref, count_ref, sems) = refs[3:8], refs[8:]
    sum_ref, left_ref, right_ref, shift_ref, rows_ref = new_refs
    masks = Masks(orbitals)
    count_copy = fetch(counts_ref, count_ref, sems.at[0])
    for place in range(lead, plan.freqs):
        sg_ref = sg_refs[place // sub - plan.lead_steps]
        prepare_frequency(
            plan, masks, place, sg_ref[0, place % sub], sg_ref[1, place % sub], place,
            left_ref, right_ref, shift_ref, rows_ref,
        )
    lefts = left_ref[pl.ds(lead * orbitals, (plan.freqs - lead) * orbitals), :]
    for item in range(plan.k_total):
        tile = hs_ref[item]
        t_ref[item] = product(lefts, right_tile(tile[:, :width], tile[:, width:]))
    left_ref[pl.ds(0, lead * orbitals), :] = old_refs[1][...]
    for old_ref, new_ref in zip(old_refs, new_refs):
        if old_ref is not old_refs[1]:
            for place in range(lead):
                new_ref[place] = old_ref[place]
    count_copy.wait()

    def one_frequency(place, carry):
        offset = pl.multiple_of((place - lead) * orbitals, orbitals)

        def store(total):
            sum_ref[place] = total

        accumulate = sum_points(
            plan, masks, rows_ref[place], shift_ref[place],
            lambda item: t_ref[item, pl.ds(offset, orbitals), :],
            hd_ref[...], wr_ref[0], jnp.zeros((orbitals, width), jnp.float32),
        )
        run_counts(count_ref[plan.freq_of(place)], accumulate, store)
        return carry

    lax.fori_loop(lead, plan.freqs, one_frequency, 0)


def far_kernel(plan, group, pieces, counts_ref, weights_ref, *refs):
    k_local, orbitals, width, freqs = plan.k_local, plan.orbitals, plan.width, plan.freqs
    half = orbitals // 2
    h_refs, refs = refs[:pieces], refs[pieces:]
    old_ref, left_ref, right_ref, shift_ref, rows_ref, wr_ref = refs[:6]
    out_ref, t_ref, hd_ref, r_ref, plane_ref, weight_ref, count_ref, sems = refs[6:]
    masks = Masks(orbitals)
    count_copy = fetch(counts_ref, count_ref, sems.at[0])
    weight_copy = fetch(weights_ref, weight_ref, sems.at[1])
    for piece in range(pieces):
        for local in range(k_local):
            place = piece * k_local + local
            matrix = h_refs[piece][local]
            hd_ref[pl.ds(place, 1), :] = diagonal_row(masks, matrix)
            tile = right_tile(*split_bf16(block_form(matrix, masks.sign)))
            t_ref[place] = product(left_ref[...], tile)
    count_copy.wait()

    def one_frequency(place, carry):
        offset = pl.multiple_of(place * orbitals, orbitals)

        def store(total):
            r_ref[place] = total

        accumulate = sum_points(
            plan, masks, rows_ref[place], shift_ref[place],
            lambda item: t_ref[item, pl.ds(offset, orbitals), :],
            hd_ref[...], wr_ref[group], old_ref[place],
        )
        run_counts(count_ref[plan.freq_of(place)], accumulate, store)
        return carry

    if pieces:
        lax.fori_loop(0, freqs, one_frequency, 0)
    totals = r_ref if pieces else old_ref
    greens = []
    for place in range(freqs):
        tile = right_ref[place]
        right = right_tile(tile[:, :width], tile[:, width:])
        greens.append(product(left_tile(*split_bf16(totals[place])), right))
    weight_copy.wait()
    norm = 1.0 / jnp.sum(weight_ref[...].astype(jnp.float32), keepdims=True)
    for place, green in enumerate(greens):
        r_ref[place] = green * norm
    for place in range(freqs):
        even = r_ref[place, pl.ds(0, half, stride=2), :]
        odd = r_ref[place, pl.ds(1, half, stride=2), :]
        plane = plan.plane_of(place)
        real_rows = pl.multiple_of(plane * half, half)
        imag_rows = pl.multiple_of((freqs + plane) * half, half)
        plane_ref[pl.ds(real_rows, half), :] = jnp.where(masks.left_row, even, swap_halves(odd))
        plane_ref[pl.ds(imag_rows, half), :] = jnp.where(masks.left_row, swap_halves(even), odd)
    for line in range(half):
        out_ref[line] = plane_ref[pl.ds(line, 2 * freqs, stride=half), :]


def local_green(hamiltonian, self_energy, guess_factor, weights, counts):
    plan = Layout(hamiltonian, self_energy)
    orbitals, width, sub, freqs = plan.orbitals, plan.width, plan.sub, plan.freqs
    x_devs, z_devs, k_local = plan.x_devs, plan.z_devs, plan.k_local
    devices = plan.freq_devs * plan.group_devs
    pair_block = orbitals * orbitals // devices
    half = orbitals // 2
    c_pos = plan.positions()[2]

    def core_flip(values):
        return lax.ppermute(values, "kgrp", [(i, i ^ 1) for i in range(plan.group_devs)])

    def x_flip(values):
        return lax.ppermute(values, "freq", [(i, i ^ 1) for i in range(plan.freq_devs)])

    def z_move(values, step):
        pairs = []
        for i in range(plan.freq_devs):
            z_pos, x_pos = i // x_devs, i % x_devs
            target = z_pos ^ step if is_power_of_two(z_devs) else (z_pos + step) % z_devs
            pairs.append((i, target * x_devs + x_pos))
        return lax.ppermute(values, "freq", pairs)

    own = jnp.stack([self_energy, guess_factor])
    own = lax.dynamic_slice_in_dim(own, c_pos * sub, sub, 1)
    others = [z_move(own, step) for step in reversed(range(plan.lead_steps, z_devs))][::-1]
    leading = [own] + [z_move(own, step) for step in range(1, plan.lead_steps)]
    near, near_flips, far, far_flips = [hamiltonian], [(0, 0)], [], []
    if plan.c_devs == 2:
        near.append(core_flip(hamiltonian))
        near_flips.append((0, 1))
    if x_devs == 2:
        crossing, _ = lax.optimization_barrier((hamiltonian, own))
        far.append(x_flip(crossing))
        far_flips.append((1, 0))
        if plan.c_devs == 2:
            far_flips.append((1, 1))
    flips = (tuple(near_flips), tuple(far_flips))
    plan.k_total = len(near) * k_local
    k_rows = -(-plan.k_total // 8) * 8

    vmem = pl.BlockSpec(memory_space=pltpu.VMEM)
    outside = pl.BlockSpec(memory_space=pltpu.HBM)

    def in_hbm(values):
        return pltpu.with_memory_space_constraint(values, pltpu.HBM)

    count_scratch = pltpu.SMEM(counts.shape, counts.dtype)
    far_counts = in_hbm(counts)
    params = pltpu.CompilerParams(vmem_limit_bytes=40 * 1024 * 1024)

    estimate = pl.CostEstimate(flops=COST, bytes_accessed=1 << 20, transcendentals=0)

    def f32(*shape):
        return jax.ShapeDtypeStruct(shape, jnp.float32)

    def bf16(*shape):
        return jax.ShapeDtypeStruct(shape, jnp.bfloat16)

    def shared(places):
        return [
            f32(places, orbitals, width),
            bf16(places * orbitals, 2 * width),
            bf16(places, 2 * orbitals, 2 * width),
            f32(places, orbitals, width),
            f32(places, 8, width),
        ]

    outputs = shared(plan.lead) + [
        bf16(plan.k_total, 2 * orbitals, 2 * width), f32(k_rows, width), f32(2, k_rows, width)
    ]
    lead = pl.pallas_call(
        functools.partial(first_kernel, plan, flips),
        out_shape=outputs,
        in_specs=[outside] * 3 + [vmem] * (len(leading) + len(near) - 1),
        out_specs=[vmem] * len(outputs),
        scratch_shapes=[
            pltpu.VMEM((plan.k_total, plan.lead * orbitals, width), jnp.float32),
            pltpu.VMEM((k_local, orbitals, width), jnp.float32),
            pltpu.SMEM(weights.shape, weights.dtype),
            count_scratch,
            pltpu.SemaphoreType.DMA((3,)),
        ],
        compiler_params=params,
        cost_estimate=estimate,
        name="first",
    )
    *old, h_tiles, h_diags, w_rows = lead(
        in_hbm(weights), far_counts, in_hbm(hamiltonian), *leading, *near[1:]
    )
    outputs = shared(freqs)
    shares = pl.pallas_call(
        functools.partial(near_kernel, plan),
        out_shape=outputs,
        in_specs=[outside] + [vmem] * (len(others) + len(old) + 3),
        out_specs=[vmem] * len(outputs),
        scratch_shapes=[
            pltpu.VMEM((plan.k_total, (freqs - plan.lead) * orbitals, width), jnp.float32),
            count_scratch,
            pltpu.SemaphoreType.DMA((1,)),
        ],
        compiler_params=pltpu.CompilerParams(vmem_limit_bytes=40 * 1024 * 1024),
        cost_estimate=estimate,
        name="near",
    )(far_counts, *others, *old, h_tiles, h_diags, w_rows)
    if far and plan.c_devs == 2:
        crossed, _ = lax.optimization_barrier((far[0], w_rows))
        far.append(core_flip(crossed))
    partial_sums = pl.pallas_call(
        functools.partial(far_kernel, plan, 1, len(far)),
        out_shape=f32(half, 2 * freqs, width),
        in_specs=[outside] * 2 + [vmem] * (len(far) + len(shares) + 1),
        out_specs=vmem,
        scratch_shapes=[
            pltpu.VMEM((plan.k_total, freqs * orbitals, width), jnp.float32),
            pltpu.VMEM((k_rows, width), jnp.float32),
            pltpu.VMEM((freqs, orbitals, width), jnp.float32),
            pltpu.VMEM((2 * freqs * half, width), jnp.float32),
            pltpu.VMEM((1, weights.size), weights.dtype),
            count_scratch,
            pltpu.SemaphoreType.DMA((2,)),
        ],
        compiler_params=params,
        name="far",
    )(far_counts, in_hbm(weights.reshape(1, -1)), *far, *shares, w_rows)

    share = width // pair_block
    outgoing = partial_sums.reshape(half, 2 * freqs, share, pair_block).transpose(0, 2, 1, 3)
    outgoing = outgoing.reshape(devices, 2 * freqs, pair_block)
    arrived = lax.all_to_all(outgoing, ("freq", "kgrp"), 0, 0, tiled=True)
    parts = arrived.reshape(z_devs, x_devs, plan.y_devs, plan.c_devs, 2, z_devs, sub, pair_block)
    result = jnp.sum(parts, (0, 2)).transpose(2, 3, 0, 1, 4, 5)
    return result.reshape(2 * plan.freq_total, pair_block).T


def solution(mesh):
    return jax.shard_map(
        local_green,
        mesh=mesh,
        in_specs=(
            P(("freq", "kgrp"), None, None),
            P("freq", None, None),
            P("freq", None, None),
            P(),
            P(),
        ),
        out_specs=P(("freq", "kgrp"), None),
        check_vma=False,
    )
```
